256 devices in a mesh: tm: 32 (over y_lo, z, core), series: 8 (over x, y_hi).
Axes of the slice: x: 4, y: 4 (y_hi: 2, y_lo: 2; y = y_hi * 2 + y_lo), z: 8, core: 2. Of those that a mesh axis runs over, the one named last changes fastest.
Arguments:
- history: bfloat16 [16, 8192, 1024], P('series', 'tm'), may hold values from -36 to 36
- lengths: int32 [16], P('series'), may hold values from 512 to 8192
- head_window: int32 [16], replicated, may hold values from 32 to 512, as said below
- input_proj: bfloat16 [1024, 3072], replicated
- output_proj: bfloat16 [1024, 1024], replicated, may hold values from -0.1875 to 0.1875
- mixer_down: bfloat16 [1024, 512], replicated, may hold values from -0.1875 to 0.1875
- mixer_up: bfloat16 [512, 1024], replicated, may hold values from -0.25 to 0.25
- series_mix: bfloat16 [16, 16], replicated, may hold values from -1.5 to 1.5
Outputs:
- layer_out: bfloat16 [16, 8192, 1024], P('series', 'tm')
The draws below stay inside these ranges and needn't reach their ends.
Inputs may be any that keep to these rules, and one draw needn't show every extreme that they name: `head_window`: some head has exactly 512.
All inputs are finite; a program needn't handle non-finite values.
Results may differ from the reference program's by a relative error of at most 0.0065.
Values may be sent and summed in bfloat16 or wider, within the bound.
A program may use at most 128 MiB of HBM per device.

```python
import jax
import jax.numpy as jnp
from jax import lax

D = 1024
HEADS = 16
MIX_WIDTH = 512
WINDOW = 512
PATCHES = 8192
SERIES = 16


def draw_history(key, part):
    base = jnp.clip(jax.random.normal(key, (SERIES, PATCHES, D), jnp.float32), -6.0, 6.0)
    return base.astype(jnp.bfloat16)


def draw_head_window(key, part):
    windows = jax.random.randint(key, (HEADS,), max(WINDOW // 16, 1), WINDOW + 1, dtype=jnp.int32)
    chosen = jax.random.randint(jax.random.fold_in(key, 7), (), 0, HEADS, dtype=jnp.int32)
    return windows.at[chosen].set(WINDOW)


def draw_input_proj(key, part):
    first = jax.random.normal(jax.random.fold_in(key, 1), (D, D), jnp.float32)
    second = jax.random.normal(jax.random.fold_in(key, 2), (D, D), jnp.float32)
    third = jax.random.normal(jax.random.fold_in(key, 3), (D, D), jnp.float32)
    keyed = 0.6 * first + 0.8 * second
    return (jnp.concatenate([first, keyed, third], axis=1) * D ** (-0.5)).astype(jnp.bfloat16)


def with_ends(result, own_key, smallest, high):
    longest = result.shape.index(max(result.shape))
    spots = []
    for shift in (0, 1):
        where = [jax.random.randint(jax.random.fold_in(own_key, axis), (), 0, length) for axis, length in enumerate(result.shape)]
        where[longest] = (where[longest] + shift) % result.shape[longest]
        spots.append(tuple(where))
    return result.at[spots[0]].set(smallest).at[spots[1]].set(high)


def normal_values(key, shape, deviation, limit, kind=jnp.bfloat16):
    result = deviation * jax.random.normal(key, shape, jnp.float32)
    return jnp.clip(result, min=-limit, max=limit).astype(kind)


def setup_inputs(seed: int = 0) -> dict:
    key_list = jax.random.split(jax.random.key(seed), 9)
    return {
        "history": draw_history(jax.random.fold_in(key_list[8], 71), 0),
        "lengths": with_ends(jax.random.randint(key_list[1], (SERIES,), WINDOW, PATCHES + 1), jax.random.fold_in(key_list[1], 1), WINDOW, PATCHES).astype(jnp.int32),
        "head_window": draw_head_window(jax.random.fold_in(key_list[8], 71), 0),
        "input_proj": draw_input_proj(jax.random.fold_in(key_list[8], 71), 0),
        "output_proj": normal_values(key_list[4], (D, D), D ** -0.5, 0.1875),
        "mixer_down": normal_values(key_list[5], (D, MIX_WIDTH), D ** -0.5, 0.1875),
        "mixer_up": normal_values(key_list[6], (MIX_WIDTH, D), MIX_WIDTH ** -0.5, 0.25),
        "series_mix": normal_values(key_list[7], (SERIES, SERIES), SERIES ** -0.5, 1.5),
    }


def attend(queries, keys_values, length, head_window, query_first, key_first):
    query_rows = queries.shape[0]
    key_rows = keys_values.shape[0]
    head_size = D // HEADS
    query_heads = queries.astype(jnp.float32).reshape(query_rows, HEADS, head_size)
    key_heads = keys_values[:, :D].astype(jnp.float32).reshape(key_rows, HEADS, head_size)
    value_heads = keys_values[:, D:].astype(jnp.float32).reshape(key_rows, HEADS, head_size)
    scores = jnp.einsum("qhd,khd->hqk", query_heads, key_heads) * (head_size ** -0.5)
    query_pos = query_first + jnp.arange(query_rows, dtype=jnp.int32)
    key_pos = key_first + jnp.arange(key_rows, dtype=jnp.int32)
    key_valid = (key_pos >= PATCHES - length) & (key_pos < PATCHES)
    distance = jnp.abs(query_pos[:, None] - key_pos[None, :])
    allowed = (distance[None, :, :] <= head_window[:, None, None]) & key_valid[None, None, :]
    scores = jnp.where(allowed, scores, -1e30)
    largest = jnp.max(scores, axis=-1, keepdims=True)
    weights = jnp.exp(scores - largest)
    totals = jnp.sum(weights, axis=-1)
    probabilities = weights.astype(jnp.bfloat16).astype(jnp.float32)
    combined = jnp.einsum("hqk,khd->qhd", probabilities, value_heads) / jnp.transpose(totals)[:, :, None]
    combined = combined.reshape(query_rows, D)
    query_valid = query_pos >= PATCHES - length
    return jnp.where(query_valid[:, None], combined, 0.0).astype(jnp.bfloat16)


def reference(history, lengths, head_window, input_proj, output_proj, mixer_down, mixer_up, series_mix):
    block_rows = min(512, PATCHES)
    block_count = PATCHES // block_rows

    def per_series(inputs):
        series_rows, length = inputs
        packed = jnp.dot(series_rows, input_proj, preferred_element_type=jnp.float32).astype(jnp.bfloat16)
        queries = packed[:, :D]
        padded = jnp.pad(packed[:, D:], ((WINDOW, WINDOW), (0, 0)))

        def per_block(block_index):
            first_row = (block_index * block_rows).astype(jnp.int32)
            query_block = lax.dynamic_slice_in_dim(queries, first_row, block_rows, 0)
            key_block = lax.dynamic_slice_in_dim(padded, first_row, block_rows + 2 * WINDOW, 0)
            return attend(query_block, key_block, length, head_window, first_row, first_row - WINDOW)

        attended = lax.map(per_block, jnp.arange(block_count, dtype=jnp.int32)).reshape(PATCHES, D)
        hidden = (series_rows.astype(jnp.float32) + jnp.dot(attended, output_proj, preferred_element_type=jnp.float32)).astype(jnp.bfloat16)
        branch = jnp.dot(hidden, mixer_down, preferred_element_type=jnp.float32).astype(jnp.bfloat16)
        return hidden, branch

    hidden, branch = lax.map(per_series, (history, lengths))
    combined = jnp.einsum("ab,bpc->apc", series_mix.astype(jnp.float32), branch.astype(jnp.float32)).astype(jnp.bfloat16)
    update = jnp.dot(combined.reshape(SERIES * PATCHES, MIX_WIDTH), mixer_up, preferred_element_type=jnp.float32)
    return (hidden.astype(jnp.float32) + update.reshape(SERIES, PATCHES, D)).astype(jnp.bfloat16)
```

```python
import functools
import math

import jax
import jax.numpy as jnp
from jax import lax
from jax.experimental import pallas as pl
from jax.experimental.pallas import tpu as pltpu
from jax.sharding import PartitionSpec as P

HEAD_SIZE = 64
PAIR = 2 * HEAD_SIZE
NEG = -1e30
FAR = 1 << 20
MESH = pl.DeviceIdType.MESH
BF16 = jnp.bfloat16
F32 = jnp.float32
SCALE = HEAD_SIZE ** -0.5 * math.log2(math.e)


def nt_dot(a, b):
    return lax.dot_general(a, b, (((1,), (1,)), ((), ())), preferred_element_type=F32)


def nn_dot(a, b):
    return jnp.dot(a, b, preferred_element_type=F32)


def layer_kernel(
    dims, lengths, window, mix, hist, wi_any, wo_any, wd_any, wu_any, out,
    X, Q, K, VO, M, L, ACC, DIST, ATT, HID, BR, RX, KR, CB, CI, HS, wi, wo, wd, wu,
    loc_sem, sib_sem, hs_sem, rs_sem, rr_sem, a1s, a1r, a2s, a2r,
):
    chips, groups = dims
    members = 2 * groups
    _, R, D = hist.shape
    B = 2 * R
    RC = R // 2
    C = BR.shape[1]
    CH = B // members
    pairs = D // PAIR
    me = lax.axis_index("tm")
    g = lax.axis_index("series")
    c = lax.rem(me, 2)
    chip = me // 2
    other = 1 - c
    sib = chip * 2 + other
    mine = g * 2 + c
    rchip = lax.rem(chip + 1, chips)
    lchip = lax.rem(chip + chips - 1, chips)
    total = chips * B

    def member(j):
        p = lax.rem(mine + j, members)
        return p, p // 2, lax.rem(p, 2)

    barrier = pltpu.get_barrier_semaphore()
    for nchip in (lchip, rchip):
        for core in range(2):
            pl.semaphore_signal(
                barrier, inc=1, device_id={"tm": nchip * 2 + core}, device_id_type=MESH
            )
    for j in range(1, members):
        _, pg, pc = member(j)
        pl.semaphore_signal(
            barrier, inc=1, device_id={"tm": chip * 2 + pc, "series": pg}, device_id_type=MESH
        )
    own_rows = pl.multiple_of(B + c * R, R)
    own_load = pltpu.make_async_copy(hist.at[c], X.at[pl.ds(own_rows, R)], loc_sem.at[0])
    own_load.start()
    loads = [
        pltpu.make_async_copy(src, dst, loc_sem.at[1 + i])
        for i, (src, dst) in enumerate(((wi_any, wi), (wo_any, wo), (wd_any, wd), (wu_any, wu)))
    ]
    for load in loads:
        load.start()
    pl.semaphore_wait(barrier, 4 + members - 1)

    sib_copy = pltpu.make_async_remote_copy(
        src_ref=hist.at[other], dst_ref=X.at[pl.ds(own_rows, R)],
        send_sem=sib_sem.at[0], recv_sem=sib_sem.at[1],
        device_id={"tm": sib}, device_id_type=MESH,
    )
    sib_copy.start()

    def halo_copy(phase, k, s):
        if phase == 0:
            target = jnp.where(c == 1, rchip, lchip)
            side = 1 - c
            kk = k + c * (1 - 2 * k)
            base = 2 * B + c * (R - 2 * B)
        else:
            target = jnp.where(c == 1, lchip, rchip)
            side = c
            kk = (1 - k) + c * (2 * k - 1)
            base = c * (2 * B + R)
        row = pl.multiple_of(base + kk * RC, RC)
        return pltpu.make_async_remote_copy(
            src_ref=hist.at[s, pl.ds(pl.multiple_of(kk * RC, RC), RC)],
            dst_ref=X.at[pl.ds(row, RC)],
            send_sem=rs_sem.at[phase, k, s], recv_sem=rr_sem.at[phase, side, k],
            device_id={"tm": target * 2 + s}, device_id_type=MESH,
        )

    def halo_arrived(phase, side, k):
        near_first = (1 - k) if side == 0 else k
        base = ((R, 2 * B), (0, 2 * B + R))[phase][side]
        pltpu.make_async_remote_copy(
            src_ref=hist.at[0, pl.ds(0, RC)],
            dst_ref=X.at[pl.ds(base + near_first * RC, RC)],
            send_sem=rs_sem.at[phase, k, 0], recv_sem=rr_sem.at[phase, side, k],
            device_id={"tm": sib}, device_id_type=MESH,
        ).wait_recv()

    near = [halo_copy(0, k, s) for k in range(2) for s in range(2)]
    far = [halo_copy(1, k, s) for k in range(2) for s in range(2)]
    for copy in near:
        copy.start()

    for p in range(pairs):
        VO[:, p * 2 * PAIR + PAIR:(p + 1) * 2 * PAIR] = jnp.ones((3 * B, PAIR), BF16)

    tile = 256

    def project(first, count, with_queries):
        rows = pl.ds(first, count)

        if with_queries:
            @pl.loop(0, D // tile)
            def _(j):
                cols = pl.ds(pl.multiple_of(j * tile, tile), tile)
                Q[:, cols] = (nn_dot(X[rows, :], wi[:, cols]) * SCALE).astype(BF16)

        @pl.loop(0, D // tile)
        def _(j):
            cols = pl.ds(pl.multiple_of(j * tile, tile), tile)
            wcols = pl.ds(pl.multiple_of(D + j * tile, tile), tile)
            K[rows, cols] = nn_dot(X[rows, :], wi[:, wcols]).astype(BF16)

        @pl.loop(0, D // tile)
        def _(j):
            wcols = pl.ds(pl.multiple_of(2 * D + j * tile, tile), tile)
            values = nn_dot(X[rows, :], wi[:, wcols]).astype(BF16)
            for i in range(tile // PAIR):
                at = pl.multiple_of((j * (tile // PAIR) + i) * 2 * PAIR, 2 * PAIR)
                VO[rows, pl.ds(at, PAIR)] = values[:, i * PAIR:(i + 1) * PAIR]

    length = lengths[c]
    first_valid = total - length

    def distances(q_first, q_count, k_ranges, at):
        column = 0
        for k_first, k_count in k_ranges:
            qi = q_first + lax.broadcasted_iota(jnp.int32, (q_count, k_count), 0)
            kj = k_first + lax.broadcasted_iota(jnp.int32, (q_count, k_count), 1)
            kpos = chip * B + kj
            valid = (kpos >= first_valid) & (kpos < total) & (kpos >= 0)
            DIST[at:at + q_count, column:column + k_count] = jnp.where(
                valid, jnp.abs(qi - kj), FAR
            )
            column += k_count

    lane = lax.broadcasted_iota(jnp.int32, (R, PAIR), 1)
    low = lane < HEAD_SIZE

    def attend(q_first, k_ranges, at, hp, first, last):
        q_rows = slice(q_first, q_first + R)
        cols = pl.ds(pl.multiple_of(hp * PAIR, PAIR), PAIR)
        vcols = pl.ds(pl.multiple_of(hp * 2 * PAIR, 2 * PAIR), 2 * PAIR)
        q = Q[q_rows, cols]
        zero = jnp.zeros_like(q)
        both = jnp.concatenate([jnp.where(low, q, zero), jnp.where(low, zero, q)], axis=0)
        pieces = []
        column = 0
        for k_first, k_count in k_ranges:
            keys = K[B + k_first:B + k_first + k_count, cols]
            s = nt_dot(both, keys)
            dist = DIST[at:at + R, column:column + k_count]
            pieces.append((
                jnp.where(dist <= window[2 * hp], s[:R], NEG),
                jnp.where(dist <= window[2 * hp + 1], s[R:], NEG),
            ))
            column += k_count
        tops = []
        for h in range(2):
            top = functools.reduce(
                jnp.maximum, [jnp.max(piece[h], axis=1, keepdims=True) for piece in pieces]
            )
            tops.append(top)
        if not first:
            old = M[q_rows, cols]
            tops = [
                jnp.maximum(tops[0], old[:, 0:1]),
                jnp.maximum(tops[1], old[:, HEAD_SIZE:HEAD_SIZE + 1]),
            ]
        new = jnp.where(low, tops[0], tops[1])
        added = None
        for (k_first, k_count), piece in zip(k_ranges, pieces):
            p = jnp.concatenate(
                [jnp.exp2(piece[0] - tops[0]), jnp.exp2(piece[1] - tops[1])], axis=0
            ).astype(BF16)
            part = nn_dot(p, VO[B + k_first:B + k_first + k_count, vcols])
            added = part if added is None else added + part
        acc = jnp.where(low, added[:R, :PAIR], added[R:, :PAIR])
        sums = jnp.where(low, added[:R, PAIR:], added[R:, PAIR:])
        if not first:
            alpha = jnp.exp2(old - new)
            acc = acc + ACC[q_rows, cols] * alpha
            sums = sums + L[q_rows, cols] * alpha
        if last:
            qpos = chip * B + q_first + lax.broadcasted_iota(jnp.int32, (R, PAIR), 0)
            ATT[q_rows, cols] = jnp.where(qpos >= first_valid, acc / sums, 0.0).astype(BF16)
        else:
            M[q_rows, cols] = new
            ACC[q_rows, cols] = acc
            L[q_rows, cols] = sums

    own_load.wait()
    sib_copy.wait_recv()
    loads[0].wait()
    project(B, B, True)
    own_keys = ((0, B),)
    distances(0, B, own_keys, 0)

    def own_stage(hp):
        for b in range(2):
            attend(b * R, own_keys, b * R, hp, True, False)

    pl.loop(0, pairs // 2)(own_stage)
    for copy in near:
        copy.wait_send()
    for copy in far:
        copy.start()
    pl.loop(pairs // 2, pairs)(own_stage)

    for k in range(2):
        for side in range(2):
            halo_arrived(0, side, k)
    project(R, R, False)
    project(2 * B, R, False)
    near_keys = ((-R, R), (B, R))
    distances(0, B, near_keys, 0)

    @pl.loop(0, pairs)
    def _(hp):
        for b in range(2):
            attend(b * R, near_keys, b * R, hp, False, False)

    n = members * CH
    row_i = lax.broadcasted_iota(jnp.int32, (n, members), 0)
    col_t = lax.broadcasted_iota(jnp.int32, (n, members), 1)
    spread = jnp.where(
        (row_i >= col_t * CH) & (row_i < (col_t + 1) * CH), 1.0, 0.0
    ).astype(BF16)
    half_mix = nn_dot(spread, mix[...]).astype(BF16)
    full_mix = nt_dot(half_mix, spread)
    i2 = lax.broadcasted_iota(jnp.int32, (n, n), 0) & (CH - 1)
    j2 = lax.broadcasted_iota(jnp.int32, (n, n), 1) & (CH - 1)
    KR[...] = jnp.where(i2 == j2, full_mix, 0.0).astype(BF16)

    far_keys = (((-B, R),), ((B + R, R),))
    for b in range(2):
        distances(b * R, R, far_keys[b], b * R)
    for k in range(2):
        for side in range(2):
            halo_arrived(1, side, k)
    project(0, R, False)
    project(2 * B + R, R, False)

    @pl.loop(0, pairs)
    def _(hp):
        for b in range(2):
            attend(b * R, far_keys[b], b * R, hp, False, True)

    loads[1].wait()

    @pl.loop(0, D // tile)
    def _(j):
        cols = pl.ds(pl.multiple_of(j * tile, tile), tile)
        HID[:, cols] = (
            X[B:2 * B, cols].astype(F32) + nn_dot(ATT[...], wo[:, cols])
        ).astype(BF16)

    hid_copy = pltpu.make_async_remote_copy(
        src_ref=HID.at[pl.ds(pl.multiple_of(other * R, R), R)], dst_ref=HS,
        send_sem=hs_sem.at[0], recv_sem=hs_sem.at[1],
        device_id={"tm": sib}, device_id_type=MESH,
    )
    hid_copy.start()
    loads[2].wait()

    @pl.loop(0, C // tile)
    def _(j):
        cols = pl.ds(pl.multiple_of(j * tile, tile), tile)
        BR[:, cols] = nn_dot(HID[...], wd[:, cols]).astype(BF16)

    slot = pl.ds(pl.multiple_of(mine * CH, CH), CH)

    def spread_copy(j):
        p, pg, pc = member(j)
        return pltpu.make_async_remote_copy(
            src_ref=BR.at[pl.ds(pl.multiple_of(pc * R + pg * CH, CH), CH)], dst_ref=RX.at[slot],
            send_sem=a1s.at[j], recv_sem=a1r.at[mine],
            device_id={"tm": chip * 2 + pc, "series": pg}, device_id_type=MESH,
        )

    spreads = [spread_copy(j) for j in range(1, members)]
    for copy in spreads:
        copy.start()
    RX[slot, :] = BR[pl.ds(pl.multiple_of(c * R + g * CH, CH), CH), :]
    for j in range(1, members):
        p, pg, pc = member(j)
        pltpu.make_async_remote_copy(
            src_ref=BR.at[pl.ds(0, CH)], dst_ref=RX.at[pl.ds(pl.multiple_of(p * CH, CH), CH)],
            send_sem=a1s.at[j], recv_sem=a1r.at[p],
            device_id={"tm": chip * 2 + pc, "series": pg}, device_id_type=MESH,
        ).wait_recv()
    mixed = nn_dot(KR[...], RX[...]).astype(BF16)
    CB[...] = mixed.reshape(members, CH, C)

    def back_copy(j):
        pg = lax.rem(g + j, groups)
        return pltpu.make_async_remote_copy(
            src_ref=CB.at[pl.ds(2 * pg, 2)],
            dst_ref=CI.at[:, pl.ds(pl.multiple_of(g * CH, CH), CH), :],
            send_sem=a2s.at[j], recv_sem=a2r.at[g],
            device_id={"series": pg}, device_id_type=MESH,
        )

    backs = [back_copy(j) for j in range(1, groups)]
    for copy in backs:
        copy.start()
    CI[:, pl.ds(pl.multiple_of(g * CH, CH), CH), :] = CB[pl.ds(2 * g, 2)]
    hid_copy.wait_recv()
    loads[3].wait()
    for j in range(1, groups):
        pg = lax.rem(g + j, groups)
        pltpu.make_async_remote_copy(
            src_ref=CB.at[pl.ds(0, 2)],
            dst_ref=CI.at[:, pl.ds(pl.multiple_of(pg * CH, CH), CH), :],
            send_sem=a2s.at[j], recv_sem=a2r.at[pg],
            device_id={"series": pg}, device_id_type=MESH,
        ).wait_recv()

    @pl.loop(0, D // tile)
    def _(j):
        cols = pl.ds(pl.multiple_of(j * tile, tile), tile)
        own_hidden = HID[pl.ds(pl.multiple_of(c * R, R), R), cols]
        out[c, :, cols] = (
            own_hidden.astype(F32) + nn_dot(CI[c], wu[:, cols])
        ).astype(BF16)
        out[other, :, cols] = (
            HS[:, cols].astype(F32) + nn_dot(CI[other], wu[:, cols])
        ).astype(BF16)

    sib_copy.wait_send()
    hid_copy.wait_send()
    for copy in far + spreads + backs:
        copy.wait_send()


def on_device(
    history, lengths, head_window, input_proj, output_proj, mixer_down, mixer_up, series_mix
):
    S, R, D = history.shape
    C = mixer_down.shape[1]
    chips = lax.axis_size("tm") // 2
    groups = lax.axis_size("series")
    members = 2 * groups
    B = 2 * R
    CH = B // members
    smem = pl.BlockSpec(memory_space=pltpu.SMEM)
    vmem = pl.BlockSpec(memory_space=pltpu.VMEM)
    hbm = pl.BlockSpec(memory_space=pl.ANY)
    dma = pltpu.SemaphoreType.DMA
    return pl.pallas_call(
        functools.partial(layer_kernel, (chips, groups)),
        out_shape=jax.ShapeDtypeStruct((S, R, D), BF16),
        in_specs=[smem, smem, vmem, hbm, hbm, hbm, hbm, hbm],
        out_specs=vmem,
        scratch_shapes=[
            pltpu.VMEM((3 * B, D), BF16),
            pltpu.VMEM((B, D), BF16),
            pltpu.VMEM((3 * B, D), BF16),
            pltpu.VMEM((3 * B, 2 * D), BF16),
            pltpu.VMEM((B, D), F32),
            pltpu.VMEM((B, D), F32),
            pltpu.VMEM((B, D), F32),
            pltpu.VMEM((B, B), jnp.int32),
            pltpu.VMEM((B, D), BF16),
            pltpu.VMEM((B, D), BF16),
            pltpu.VMEM((B, C), BF16),
            pltpu.VMEM((members * CH, C), BF16),
            pltpu.VMEM((members * CH, members * CH), BF16),
            pltpu.VMEM((members, CH, C), BF16),
            pltpu.VMEM((2, R, C), BF16),
            pltpu.VMEM((R, D), BF16),
            pltpu.VMEM(input_proj.shape, BF16),
            pltpu.VMEM(output_proj.shape, BF16),
            pltpu.VMEM(mixer_down.shape, BF16),
            pltpu.VMEM(mixer_up.shape, BF16),
            dma((5,)), dma((2,)), dma((2,)), dma((2, 2, 2)), dma((2, 2, 2)),
            dma((members,)), dma((members,)), dma((groups,)), dma((groups,)),
        ],
        compiler_params=pltpu.CompilerParams(
            collective_id=0, has_side_effects=True, vmem_limit_bytes=64 * 1024 * 1024 - 65536
        ),
        name="layer",
    )(lengths, head_window, series_mix, history, input_proj, output_proj, mixer_down, mixer_up)


def solution(mesh):
    in_specs = (P("series", "tm", None), P("series"), P(), P(), P(), P(), P(), P())
    out_specs = P("series", "tm", None)
    return jax.shard_map(
        on_device, mesh=mesh, in_specs=in_specs, out_specs=out_specs, check_vma=False
    )
```

```python
import functools
import math

import jax
import jax.numpy as jnp
from jax import lax
from jax.experimental import pallas as pl
from jax.experimental.pallas import tpu as pltpu
from jax.sharding import PartitionSpec as P

HEAD_SIZE = 64
PAIR = 2 * HEAD_SIZE
NEG = -1e30
FAR = 1 << 20
MESH = pl.DeviceIdType.MESH
BF16 = jnp.bfloat16
F32 = jnp.float32
SCALE = HEAD_SIZE ** -0.5 * math.log2(math.e)


def nt_dot(a, b):
    return lax.dot_general(a, b, (((1,), (1,)), ((), ())), preferred_element_type=F32)


def nn_dot(a, b):
    return jnp.dot(a, b, preferred_element_type=F32)


def layer_kernel(
    dims, lengths, window, mix, hist, wi_any, wo_any, wd_any, wu_any, out,
    X, Q, K, VO, M, L, ACC, DIST, DMID, DOUT, S0, S1, T0, T1, ATT, HID, BR, RX, KR, CB, CI, HS,
    wi, wo, wd, wu,
    loc_sem, sib_sem, hs_sem, rs_sem, rr_sem, a1s, a1r, a2s, a2r,
):
    chips, groups = dims
    members = 2 * groups
    _, R, D = hist.shape
    B = 2 * R
    RC = R // 2
    C = BR.shape[1]
    CH = RC // groups
    pairs = D // PAIR
    me = lax.axis_index("tm")
    g = lax.axis_index("series")
    c = lax.rem(me, 2)
    chip = me // 2
    other = 1 - c
    sib = chip * 2 + other
    mine = g * 2 + c
    rchip = lax.rem(chip + 1, chips)
    lchip = lax.rem(chip + chips - 1, chips)
    total = chips * B
    has_left = chip > 0
    has_right = chip < chips - 1

    def member(j):
        p = lax.rem(mine + j, members)
        return p, p // 2, lax.rem(p, 2)

    barrier = pltpu.get_barrier_semaphore()
    for nchip in (lchip, rchip):
        for core in range(2):
            pl.semaphore_signal(
                barrier, inc=1, device_id={"tm": nchip * 2 + core}, device_id_type=MESH
            )
    for j in range(1, members):
        _, pg, pc = member(j)
        pl.semaphore_signal(
            barrier, inc=1, device_id={"tm": chip * 2 + pc, "series": pg}, device_id_type=MESH
        )
    own_rows = pl.multiple_of(B + c * R, R)
    own_load = pltpu.make_async_copy(hist.at[c], X.at[pl.ds(own_rows, R)], loc_sem.at[0])
    own_load.start()
    loads = [
        pltpu.make_async_copy(src, dst, loc_sem.at[1 + i])
        for i, (src, dst) in enumerate(((wi_any, wi), (wo_any, wo), (wd_any, wd), (wu_any, wu)))
    ]
    loads[0].start()
    pl.semaphore_wait(barrier, 4 + members - 1)

    sib_copy = pltpu.make_async_remote_copy(
        src_ref=hist.at[other], dst_ref=X.at[pl.ds(own_rows, R)],
        send_sem=sib_sem.at[0], recv_sem=sib_sem.at[1],
        device_id={"tm": sib}, device_id_type=MESH,
    )
    sib_copy.start()

    sends = (
        jnp.where(c == 1, has_right, has_left),
        jnp.where(c == 1, has_left, has_right),
    )

    def halo_copy(phase, k, s):
        if phase == 0:
            target = jnp.where(c == 1, rchip, lchip)
            side = 1 - c
            kk = k + c * (1 - 2 * k)
            base = 2 * B + c * (R - 2 * B)
        else:
            target = jnp.where(c == 1, lchip, rchip)
            side = c
            kk = (1 - k) + c * (2 * k - 1)
            base = c * (2 * B + R)
        row = pl.multiple_of(base + kk * RC, RC)
        return pltpu.make_async_remote_copy(
            src_ref=hist.at[s, pl.ds(pl.multiple_of(kk * RC, RC), RC)],
            dst_ref=X.at[pl.ds(row, RC)],
            send_sem=rs_sem.at[phase, k, s], recv_sem=rr_sem.at[phase, side, k],
            device_id={"tm": target * 2 + s}, device_id_type=MESH,
        )

    def halo_row(phase, side, k):
        base = ((R, 2 * B), (0, 2 * B + R))[phase][side]
        return base + ((1 - k) if side == 0 else k) * RC

    def halo_arrived(phase, k):
        for side in range(2):
            @pl.when((has_left, has_right)[side])
            def _():
                pltpu.make_async_remote_copy(
                    src_ref=hist.at[0, pl.ds(0, RC)],
                    dst_ref=X.at[pl.ds(halo_row(phase, side, k), RC)],
                    send_sem=rs_sem.at[phase, k, 0], recv_sem=rr_sem.at[phase, side, k],
                    device_id={"tm": sib}, device_id_type=MESH,
                ).wait_recv()

    def start_halo(phase):
        @pl.when(sends[phase])
        def _():
            for k in range(2):
                for s in range(2):
                    halo_copy(phase, k, s).start()

    def halo_sent(phase, k):
        @pl.when(sends[phase])
        def _():
            for s in range(2):
                halo_copy(phase, k, s).wait_send()

    start_halo(0)
    for load in loads[1:]:
        load.start()

    @pl.when(jnp.logical_not(has_left))
    def _():
        X[0:B, :] = jnp.zeros((B, D), BF16)

    @pl.when(jnp.logical_not(has_right))
    def _():
        X[2 * B:3 * B, :] = jnp.zeros((B, D), BF16)

    for p in range(pairs):
        VO[:, p * 2 * PAIR + PAIR:(p + 1) * 2 * PAIR] = jnp.ones((3 * B, PAIR), BF16)

    tile = 256

    def stacked(ref, rows, cols=slice(None)):
        parts = [ref[first:first + count, cols] for first, count in rows]
        return parts[0] if len(parts) == 1 else jnp.concatenate(parts, axis=0)

    def scatter(ref, rows, cols, value):
        at = 0
        for first, count in rows:
            ref[first:first + count, cols] = value[at:at + count]
            at += count

    def project(rows, with_queries):
        @pl.loop(0, D // tile)
        def _(j):
            cols = pl.ds(pl.multiple_of(j * tile, tile), tile)
            x = stacked(X, rows)
            if with_queries:
                Q[:, cols] = (nn_dot(x, wi[:, cols]) * SCALE).astype(BF16)
            kcols = pl.ds(pl.multiple_of(D + j * tile, tile), tile)
            scatter(K, rows, cols, nn_dot(x, wi[:, kcols]).astype(BF16))
            wcols = pl.ds(pl.multiple_of(2 * D + j * tile, tile), tile)
            values = nn_dot(x, wi[:, wcols]).astype(BF16)
            for i in range(tile // PAIR):
                at = pl.multiple_of((j * (tile // PAIR) + i) * 2 * PAIR, 2 * PAIR)
                scatter(VO, rows, pl.ds(at, PAIR), values[:, i * PAIR:(i + 1) * PAIR])

    length = lengths[c]
    first_valid = total - length

    def distances(ref, at, unit):
        q_first, n, k_ranges = unit[:3]
        column = 0
        for k_first, k_count in k_ranges:
            qi = q_first + lax.broadcasted_iota(jnp.int32, (n, k_count), 0)
            kj = k_first + lax.broadcasted_iota(jnp.int32, (n, k_count), 1)
            kpos = chip * B + kj
            valid = (kpos >= first_valid) & (kpos < total) & (kpos >= 0)
            ref[at:at + n, column:column + k_count] = jnp.where(valid, jnp.abs(qi - kj), FAR)
            column += k_count

    def pair_cols(hp):
        return pl.ds(pl.multiple_of(hp * PAIR, PAIR), PAIR)

    def scores(unit, hp, S, T):
        q_first, n, k_ranges, ref, at = unit
        low = lax.broadcasted_iota(jnp.int32, (n, PAIR), 1) < HEAD_SIZE
        cols = pair_cols(hp)
        q = Q[q_first:q_first + n, cols]
        zero = jnp.zeros_like(q)
        both = jnp.concatenate([jnp.where(low, q, zero), jnp.where(low, zero, q)], axis=0)
        tops = []
        column = 0
        for k_first, k_count in k_ranges:
            s = nt_dot(both, K[B + k_first:B + k_first + k_count, cols])
            dist = ref[at:at + n, column:column + k_count]
            s = jnp.concatenate([
                jnp.where(dist <= window[2 * hp], s[:n], NEG),
                jnp.where(dist <= window[2 * hp + 1], s[n:], NEG),
            ], axis=0)
            S[:2 * n, column:column + k_count] = s
            tops.append(jnp.max(s, axis=1, keepdims=True))
            column += k_count
        top = functools.reduce(jnp.maximum, tops)
        T[:2 * n, :] = jnp.broadcast_to(top, (2 * n, PAIR))

    def values(unit, hp, S, T, first, last):
        q_first, n, k_ranges, _, _ = unit
        low = lax.broadcasted_iota(jnp.int32, (n, PAIR), 1) < HEAD_SIZE
        cols = pair_cols(hp)
        vcols = pl.ds(pl.multiple_of(hp * 2 * PAIR, 2 * PAIR), 2 * PAIR)
        q_rows = slice(q_first, q_first + n)
        top = T[:2 * n, :]
        if not first:
            old = jnp.concatenate([M[hp, 0, q_rows, :], M[hp, 1, q_rows, :]], axis=0)
            top = jnp.maximum(top, old)
        added = None
        column = 0
        for k_first, k_count in k_ranges:
            step = min(PAIR, k_count)
            p = jnp.concatenate([
                jnp.exp2(S[:2 * n, column + i:column + i + step] - top[:, :step]).astype(BF16)
                for i in range(0, k_count, step)
            ], axis=1)
            part = nn_dot(p, VO[B + k_first:B + k_first + k_count, vcols])
            added = part if added is None else added + part
            column += k_count
        acc = jnp.where(low, added[:n, :PAIR], added[n:, :PAIR])
        sums = jnp.where(low, added[:n, PAIR:], added[n:, PAIR:])
        if not first:
            alpha = jnp.exp2(jnp.where(low, old[:n] - top[:n], old[n:] - top[n:]))
            acc = acc + ACC[q_rows, cols] * alpha
            sums = sums + L[q_rows, cols] * alpha
        if last:
            qpos = chip * B + q_first + lax.broadcasted_iota(jnp.int32, (n, PAIR), 0)
            ATT[q_rows, cols] = jnp.where(qpos >= first_valid, acc / sums, 0.0).astype(BF16)
        else:
            M[hp, 0, q_rows, :] = top[:n]
            M[hp, 1, q_rows, :] = top[n:]
            ACC[q_rows, cols] = acc
            L[q_rows, cols] = sums

    def attend(units, first, last):
        scores(units[0], 0, S0, T0)

        @pl.loop(0, pairs)
        def _(hp):
            scores(units[1], hp, S1, T1)
            values(units[0], hp, S0, T0, first, last)
            scores(units[0], jnp.minimum(hp + 1, pairs - 1), S0, T0)
            values(units[1], hp, S1, T1, first, last)

    own_load.wait()
    sib_copy.wait_recv()
    loads[0].wait()
    project([(B, B)], True)
    halo_sent(0, 0)
    start_halo(1)
    own = [(b * R, R, ((0, B),), DIST, b * R) for b in range(2)]
    for unit in own:
        distances(DIST, unit[4], unit)
    attend(own, True, False)

    for k in range(2):
        halo_arrived(0, k)
    project([(R, R), (2 * B, R)], False)
    near = [(b * R, R, ((-R, R), (B, R)), DIST, b * R) for b in range(2)]
    for unit in near:
        distances(DIST, unit[4], unit)
    attend(near, False, False)

    n = members * CH
    row_i = lax.broadcasted_iota(jnp.int32, (n, members), 0)
    col_t = lax.broadcasted_iota(jnp.int32, (n, members), 1)
    spread = jnp.where(
        (row_i >= col_t * CH) & (row_i < (col_t + 1) * CH), 1.0, 0.0
    ).astype(BF16)
    half_mix = nn_dot(spread, mix[...]).astype(BF16)
    full_mix = nt_dot(half_mix, spread)
    i2 = lax.broadcasted_iota(jnp.int32, (n, n), 0) & (CH - 1)
    j2 = lax.broadcasted_iota(jnp.int32, (n, n), 1) & (CH - 1)
    KR[...] = jnp.where(i2 == j2, full_mix, 0.0).astype(BF16)

    far_mid = [
        (RC, RC, ((-B + RC, RC),), DMID, 0),
        (R, RC, ((B + R, RC),), DMID, RC),
    ]
    far_out = [
        (0, RC, ((-B, R),), DOUT, 0),
        (R + RC, RC, ((B + R, R),), DOUT, RC),
    ]
    for unit in far_mid + far_out:
        distances(unit[3], unit[4], unit)

    def rows_of(group, core):
        return (RC + core * RC) if group == 0 else core * (R + RC)

    def spread_copy(group, j):
        p, pg, pc = member(j)
        row = pl.multiple_of(rows_of(group, pc) + pg * CH, CH)
        return pltpu.make_async_remote_copy(
            src_ref=BR.at[pl.ds(row, CH)],
            dst_ref=RX.at[group, pl.ds(pl.multiple_of(mine * CH, CH), CH)],
            send_sem=a1s.at[group, j], recv_sem=a1r.at[group, mine],
            device_id={"tm": chip * 2 + pc, "series": pg}, device_id_type=MESH,
        )

    def spread_arrived(group, j):
        p, pg, pc = member(j)
        pltpu.make_async_remote_copy(
            src_ref=BR.at[pl.ds(0, CH)],
            dst_ref=RX.at[group, pl.ds(pl.multiple_of(p * CH, CH), CH)],
            send_sem=a1s.at[group, j], recv_sem=a1r.at[group, p],
            device_id={"tm": chip * 2 + pc, "series": pg}, device_id_type=MESH,
        ).wait_recv()

    def local_rows(group, core):
        return rows_of(group, core) - core * R

    def back_copy(group, j):
        pg = lax.rem(g + j, groups)
        row = pl.multiple_of(local_rows(group, c) + g * CH, CH)
        return pltpu.make_async_remote_copy(
            src_ref=CB.at[group, pl.ds(2 * pg, 2)],
            dst_ref=CI.at[:, pl.ds(row, CH), :],
            send_sem=a2s.at[group, j], recv_sem=a2r.at[group, g],
            device_id={"series": pg}, device_id_type=MESH,
        )

    def back_arrived(group, j):
        pg = lax.rem(g + j, groups)
        row = pl.multiple_of(local_rows(group, c) + pg * CH, CH)
        pltpu.make_async_remote_copy(
            src_ref=CB.at[group, pl.ds(0, 2)],
            dst_ref=CI.at[:, pl.ds(row, CH), :],
            send_sem=a2s.at[group, j], recv_sem=a2r.at[group, pg],
            device_id={"series": pg}, device_id_type=MESH,
        ).wait_recv()

    def hidden_copy(group):
        src = pl.multiple_of(rows_of(group, other), RC)
        dst = pl.multiple_of(local_rows(group, other), RC)
        return pltpu.make_async_remote_copy(
            src_ref=HID.at[pl.ds(src, RC)], dst_ref=HS.at[pl.ds(dst, RC)],
            send_sem=hs_sem.at[group, 0], recv_sem=hs_sem.at[group, 1],
            device_id={"tm": sib}, device_id_type=MESH,
        )

    def finish_rows(group, rows):
        @pl.loop(0, D // tile)
        def _(j):
            cols = pl.ds(pl.multiple_of(j * tile, tile), tile)
            own_x = stacked(X, [(B + first, count) for first, count in rows], cols)
            update = nn_dot(stacked(ATT, rows), wo[:, cols])
            scatter(HID, rows, cols, (own_x.astype(F32) + update).astype(BF16))

        hidden_copy(group).start()

        @pl.loop(0, C // tile)
        def _(j):
            cols = pl.ds(pl.multiple_of(j * tile, tile), tile)
            scatter(BR, rows, cols, nn_dot(stacked(HID, rows), wd[:, cols]).astype(BF16))

        for j in range(1, members):
            spread_copy(group, j).start()
        row = pl.multiple_of(rows_of(group, c) + g * CH, CH)
        RX[group, pl.ds(pl.multiple_of(mine * CH, CH), CH), :] = BR[pl.ds(row, CH), :]

    def mix_rows(group):
        for j in range(1, members):
            spread_arrived(group, j)
        CB[group] = nn_dot(KR[...], RX[group]).astype(BF16).reshape(members, CH, C)
        for j in range(1, groups):
            back_copy(group, j).start()
        row = pl.multiple_of(local_rows(group, c) + g * CH, CH)
        CI[:, pl.ds(row, CH), :] = CB[group, pl.ds(2 * g, 2)]

    def put_rows(group):
        hidden_copy(group).wait_recv()
        for j in range(1, groups):
            back_arrived(group, j)
        from_row = pl.multiple_of(rows_of(group, c), RC)
        at_row = pl.multiple_of(local_rows(group, c), RC)
        rows = pl.ds(at_row, RC)

        @pl.loop(0, D // tile)
        def _(j):
            cols = pl.ds(pl.multiple_of(j * tile, tile), tile)
            sums = jnp.concatenate([CI[c, rows, :], CI[other, rows, :]], axis=0)
            update = nn_dot(sums, wu[:, cols])
            out[c, rows, cols] = (
                HID[pl.ds(from_row, RC), cols].astype(F32) + update[:RC]
            ).astype(BF16)
            out[other, rows, cols] = (HS[rows, cols].astype(F32) + update[RC:]).astype(BF16)

    mid_rows = [(RC, R)]
    out_rows = [(0, RC), (R + RC, RC)]
    halo_arrived(1, 0)
    project([(halo_row(1, 0, 0), RC), (halo_row(1, 1, 0), RC)], False)
    attend(far_mid, False, True)
    loads[1].wait()
    loads[2].wait()
    finish_rows(0, mid_rows)
    halo_arrived(1, 1)
    project([(halo_row(1, 0, 1), RC), (halo_row(1, 1, 1), RC)], False)
    attend(far_out, False, True)
    finish_rows(1, out_rows)
    mix_rows(0)
    mix_rows(1)
    loads[3].wait()
    put_rows(0)
    put_rows(1)

    sib_copy.wait_send()
    halo_sent(0, 1)
    for k in range(2):
        halo_sent(1, k)
    for group in range(2):
        hidden_copy(group).wait_send()
        for j in range(1, members):
            spread_copy(group, j).wait_send()
        for j in range(1, groups):
            back_copy(group, j).wait_send()


def on_device(
    history, lengths, head_window, input_proj, output_proj, mixer_down, mixer_up, series_mix
):
    S, R, D = history.shape
    C = mixer_down.shape[1]
    chips = lax.axis_size("tm") // 2
    groups = lax.axis_size("series")
    members = 2 * groups
    B = 2 * R
    RC = R // 2
    CH = RC // groups
    pairs = D // PAIR
    smem = pl.BlockSpec(memory_space=pltpu.SMEM)
    vmem = pl.BlockSpec(memory_space=pltpu.VMEM)
    hbm = pl.BlockSpec(memory_space=pl.ANY)
    dma = pltpu.SemaphoreType.DMA
    return pl.pallas_call(
        functools.partial(layer_kernel, (chips, groups)),
        out_shape=jax.ShapeDtypeStruct((S, R, D), BF16),
        in_specs=[smem, smem, vmem, hbm, hbm, hbm, hbm, hbm],
        out_specs=vmem,
        scratch_shapes=[
            pltpu.VMEM((3 * B, D), BF16),
            pltpu.VMEM((B, D), BF16),
            pltpu.VMEM((3 * B, D), BF16),
            pltpu.VMEM((3 * B, 2 * D), BF16),
            pltpu.VMEM((pairs, 2, B, PAIR), F32),
            pltpu.VMEM((B, D), F32),
            pltpu.VMEM((B, D), F32),
            pltpu.VMEM((B, B), jnp.int32),
            pltpu.VMEM((R, RC), jnp.int32),
            pltpu.VMEM((R, R), jnp.int32),
            pltpu.VMEM((B, B), F32),
            pltpu.VMEM((B, B), F32),
            pltpu.VMEM((B, PAIR), F32),
            pltpu.VMEM((B, PAIR), F32),
            pltpu.VMEM((B, D), BF16),
            pltpu.VMEM((B, D), BF16),
            pltpu.VMEM((B, C), BF16),
            pltpu.VMEM((2, members * CH, C), BF16),
            pltpu.VMEM((members * CH, members * CH), BF16),
            pltpu.VMEM((2, members, CH, C), BF16),
            pltpu.VMEM((2, R, C), BF16),
            pltpu.VMEM((R, D), BF16),
            pltpu.VMEM(input_proj.shape, BF16),
            pltpu.VMEM(output_proj.shape, BF16),
            pltpu.VMEM(mixer_down.shape, BF16),
            pltpu.VMEM(mixer_up.shape, BF16),
            dma((5,)), dma((2,)), dma((2, 2)), dma((2, 2, 2)), dma((2, 2, 2)),
            dma((2, members)), dma((2, members)), dma((2, groups)), dma((2, groups)),
        ],
        compiler_params=pltpu.CompilerParams(
            collective_id=0, has_side_effects=True, vmem_limit_bytes=64 * 1024 * 1024 - 65536
        ),
        name="layer",
    )(lengths, head_window, series_mix, history, input_proj, output_proj, mixer_down, mixer_up)


def solution(mesh):
    in_specs = (P("series", "tm", None), P("series"), P(), P(), P(), P(), P(), P())
    out_specs = P("series", "tm", None)
    return jax.shard_map(
        on_device, mesh=mesh, in_specs=in_specs, out_specs=out_specs, check_vma=False
    )
```

```python
import functools
import math

import jax
import jax.numpy as jnp
from jax import lax
from jax.experimental import pallas as pl
from jax.experimental.pallas import tpu as pltpu
from jax.sharding import PartitionSpec as P

HEAD_SIZE = 64
PAIR = 2 * HEAD_SIZE
NEG = -1e30
FAR = 1 << 20
MESH = pl.DeviceIdType.MESH
BF16 = jnp.bfloat16
F32 = jnp.float32
SCALE = HEAD_SIZE ** -0.5 * math.log2(math.e)


def nt_dot(a, b):
    return lax.dot_general(a, b, (((1,), (1,)), ((), ())), preferred_element_type=F32)


def nn_dot(a, b):
    return jnp.dot(a, b, preferred_element_type=F32)


def layer_kernel(
    dims, lengths, window, mix, hist, wi_any, wo_any, wd_any, hid_out, mix_out,
    X, Q, K, VO, M, L, ACC, DIST, DMID, DOUT, S0, S1, T0, T1, ATT, HID, BR, RX, KR, CB,
    wi, wo, wd,
    loc_sem, sib_sem, hs_sem, rs_sem, rr_sem, a1s, a1r, a2s, a2r,
):
    chips, groups = dims
    members = 2 * groups
    _, R, D = hist.shape
    B = 2 * R
    RC = R // 2
    C = BR.shape[1]
    CH = RC // groups
    pairs = D // PAIR
    me = lax.axis_index("tm")
    g = lax.axis_index("series")
    c = lax.rem(me, 2)
    chip = me // 2
    other = 1 - c
    sib = chip * 2 + other
    mine = g * 2 + c
    rchip = lax.rem(chip + 1, chips)
    lchip = lax.rem(chip + chips - 1, chips)
    total = chips * B
    has_left = chip > 0
    has_right = chip < chips - 1

    def member(j):
        p = lax.rem(mine + j, members)
        return p, p // 2, lax.rem(p, 2)

    barrier = pltpu.get_barrier_semaphore()
    for nchip in (lchip, rchip):
        for core in range(2):
            pl.semaphore_signal(
                barrier, inc=1, device_id={"tm": nchip * 2 + core}, device_id_type=MESH
            )
    for j in range(1, members):
        _, pg, pc = member(j)
        pl.semaphore_signal(
            barrier, inc=1, device_id={"tm": chip * 2 + pc, "series": pg}, device_id_type=MESH
        )
    own_rows = pl.multiple_of(c * R, R)
    own_load = pltpu.make_async_copy(hist.at[c], X.at[pl.ds(own_rows, R)], loc_sem.at[0])
    own_load.start()
    loads = [
        pltpu.make_async_copy(src, dst, loc_sem.at[1 + i])
        for i, (src, dst) in enumerate(((wi_any, wi), (wo_any, wo), (wd_any, wd)))
    ]
    loads[0].start()
    pl.semaphore_wait(barrier, 4 + members - 1)

    sib_copy = pltpu.make_async_remote_copy(
        src_ref=hist.at[other], dst_ref=X.at[pl.ds(own_rows, R)],
        send_sem=sib_sem.at[0], recv_sem=sib_sem.at[1],
        device_id={"tm": sib}, device_id_type=MESH,
    )
    sib_copy.start()

    sends = (
        jnp.where(c == 1, has_right, has_left),
        jnp.where(c == 1, has_left, has_right),
    )

    def halo_copy(phase, k, s):
        if phase == 0:
            target = jnp.where(c == 1, rchip, lchip)
            side = 1 - c
            kk = k + c * (1 - 2 * k)
            base = B + side * R
        else:
            target = jnp.where(c == 1, lchip, rchip)
            side = c
            kk = (1 - k) + c * (2 * k - 1)
            base = 2 * B + side * R
        row = pl.multiple_of(base + kk * RC, RC)
        return pltpu.make_async_remote_copy(
            src_ref=hist.at[s, pl.ds(pl.multiple_of(kk * RC, RC), RC)],
            dst_ref=X.at[pl.ds(row, RC)],
            send_sem=rs_sem.at[phase, k, s], recv_sem=rr_sem.at[phase, side, k],
            device_id={"tm": target * 2 + s}, device_id_type=MESH,
        )

    def halo_row(phase, side, k):
        return (phase + 1) * B + side * R + ((1 - k) if side == 0 else k) * RC

    def halo_arrived(phase, k):
        for side in range(2):
            @pl.when((has_left, has_right)[side])
            def _():
                pltpu.make_async_remote_copy(
                    src_ref=hist.at[0, pl.ds(0, RC)],
                    dst_ref=X.at[pl.ds(halo_row(phase, side, k), RC)],
                    send_sem=rs_sem.at[phase, k, 0], recv_sem=rr_sem.at[phase, side, k],
                    device_id={"tm": sib}, device_id_type=MESH,
                ).wait_recv()

    def start_halo(phase):
        @pl.when(sends[phase])
        def _():
            for k in range(2):
                for s in range(2):
                    halo_copy(phase, k, s).start()

    def halo_sent(phase, k):
        @pl.when(sends[phase])
        def _():
            for s in range(2):
                halo_copy(phase, k, s).wait_send()

    start_halo(0)
    for load in loads[1:]:
        load.start()

    @pl.when(jnp.logical_not(has_left))
    def _():
        for phase in range(1, 3):
            X[phase * B:phase * B + R, :] = jnp.zeros((R, D), BF16)

    @pl.when(jnp.logical_not(has_right))
    def _():
        for phase in range(1, 3):
            X[phase * B + R:(phase + 1) * B, :] = jnp.zeros((R, D), BF16)

    for p in range(pairs):
        VO[:, p * 2 * PAIR + PAIR:(p + 1) * 2 * PAIR] = jnp.ones((3 * B, PAIR), BF16)

    tile = 256

    def stacked(ref, rows, cols=slice(None)):
        parts = [ref[first:first + count, cols] for first, count in rows]
        return parts[0] if len(parts) == 1 else jnp.concatenate(parts, axis=0)

    def scatter(ref, rows, cols, value):
        at = 0
        for first, count in rows:
            ref[first:first + count, cols] = value[at:at + count]
            at += count

    def project(rows, with_queries):
        @pl.loop(0, D // tile)
        def _(j):
            cols = pl.ds(pl.multiple_of(j * tile, tile), tile)
            x = stacked(X, rows)
            if with_queries:
                Q[:, cols] = (nn_dot(x, wi[:, cols]) * SCALE).astype(BF16)
            kcols = pl.ds(pl.multiple_of(D + j * tile, tile), tile)
            scatter(K, rows, cols, nn_dot(x, wi[:, kcols]).astype(BF16))
            wcols = pl.ds(pl.multiple_of(2 * D + j * tile, tile), tile)
            values = nn_dot(x, wi[:, wcols]).astype(BF16)
            for i in range(tile // PAIR):
                at = pl.multiple_of((j * (tile // PAIR) + i) * 2 * PAIR, 2 * PAIR)
                scatter(VO, rows, pl.ds(at, PAIR), values[:, i * PAIR:(i + 1) * PAIR])

    length = lengths[c]
    first_valid = total - length

    def distances(unit):
        q_first, n, _, segments, ref, at = unit
        column = 0
        for k_first, k_count in segments:
            qi = q_first + lax.broadcasted_iota(jnp.int32, (n, k_count), 0)
            kj = k_first + lax.broadcasted_iota(jnp.int32, (n, k_count), 1)
            kpos = chip * B + kj
            valid = (kpos >= first_valid) & (kpos < total) & (kpos >= 0)
            ref[at:at + n, column:column + k_count] = jnp.where(valid, jnp.abs(qi - kj), FAR)
            column += k_count

    def pair_cols(hp):
        return pl.ds(pl.multiple_of(hp * PAIR, PAIR), PAIR)

    def scores(unit, hp, S, T, r0=0):
        q_first, n, k_row, segments, ref, at = unit
        count = sum(k_count for _, k_count in segments)
        low = lax.broadcasted_iota(jnp.int32, (n, PAIR), 1) < HEAD_SIZE
        cols = pair_cols(hp)
        q = Q[q_first:q_first + n, cols]
        zero = jnp.zeros_like(q)
        both = jnp.concatenate([jnp.where(low, q, zero), jnp.where(low, zero, q)], axis=0)
        s = nt_dot(both, K[k_row:k_row + count, cols])
        dist = ref[at:at + n, :count]
        s = jnp.concatenate([
            jnp.where(dist <= window[2 * hp], s[:n], NEG),
            jnp.where(dist <= window[2 * hp + 1], s[n:], NEG),
        ], axis=0)
        S[r0:r0 + 2 * n, :count] = s
        top = jnp.max(s, axis=1, keepdims=True)
        T[r0:r0 + 2 * n, :] = jnp.broadcast_to(top, (2 * n, PAIR))

    def values(unit, hp, S, T, first, last, r0=0):
        q_first, n, k_row, segments, _, _ = unit
        count = sum(k_count for _, k_count in segments)
        low = lax.broadcasted_iota(jnp.int32, (n, PAIR), 1) < HEAD_SIZE
        cols = pair_cols(hp)
        vcols = pl.ds(pl.multiple_of(hp * 2 * PAIR, 2 * PAIR), 2 * PAIR)
        q_rows = slice(q_first, q_first + n)
        top = T[r0:r0 + 2 * n, :]
        if not first:
            old = jnp.concatenate([M[hp, 0, q_rows, :], M[hp, 1, q_rows, :]], axis=0)
            top = jnp.maximum(top, old)
        step = min(PAIR, count)
        p = jnp.concatenate([
            jnp.exp2(S[r0:r0 + 2 * n, i:i + step] - top[:, :step]).astype(BF16)
            for i in range(0, count, step)
        ], axis=1)
        added = nn_dot(p, VO[k_row:k_row + count, vcols])
        acc = jnp.where(low, added[:n, :PAIR], added[n:, :PAIR])
        sums = jnp.where(low, added[:n, PAIR:], added[n:, PAIR:])
        if not first:
            alpha = jnp.exp2(jnp.where(low, old[:n] - top[:n], old[n:] - top[n:]))
            acc = acc + ACC[q_rows, cols] * alpha
            sums = sums + L[q_rows, cols] * alpha
        if last:
            qpos = chip * B + q_first + lax.broadcasted_iota(jnp.int32, (n, PAIR), 0)
            ATT[q_rows, cols] = jnp.where(qpos >= first_valid, acc / sums, 0.0).astype(BF16)
        else:
            M[hp, 0, q_rows, :] = top[:n]
            M[hp, 1, q_rows, :] = top[n:]
            ACC[q_rows, cols] = acc
            L[q_rows, cols] = sums

    def attend(units, first, last):
        if len(units) == 4:
            batches = [
                [(unit, 0, 2 * RC * b) for b, unit in enumerate(units[2 * i:2 * i + 2])]
                for i in range(2)
            ]
            step = 1
        elif units[0][1] == R:
            batches = [[(units[0], 0, 0)], [(units[1], 0, 0)]]
            step = 1
        else:
            batches = [[(unit, i, 2 * RC * b) for b, unit in enumerate(units)] for i in range(2)]
            step = 2

        def all_scores(batch, hp, S, T):
            for unit, plus, r0 in batch:
                scores(unit, hp + plus, S, T, r0)

        def all_values(batch, hp, S, T):
            for unit, plus, r0 in batch:
                values(unit, hp + plus, S, T, first, last, r0)

        all_scores(batches[0], 0, S0, T0)

        @pl.loop(0, pairs // step)
        def _(i):
            hp = i * step
            all_scores(batches[1], hp, S1, T1)
            all_values(batches[0], hp, S0, T0)
            all_scores(batches[0], jnp.minimum(hp + step, pairs - step), S0, T0)
            all_values(batches[1], hp, S1, T1)

    own_load.wait()
    sib_copy.wait_recv()
    loads[0].wait()
    project([(0, B)], True)
    halo_sent(0, 0)
    start_halo(1)
    own = [(b * R, R, 0, ((0, B),), DIST, b * R) for b in range(2)]
    for unit in own:
        distances(unit)
    attend(own, True, False)

    for k in range(2):
        halo_arrived(0, k)
    project([(B, B)], False)
    near = [
        (0, RC, B, ((-R, R), (B, RC)), DIST, 0),
        (RC, RC, B, ((-R, R), (B, R)), DIST, RC),
        (R, RC, B, ((-R, R), (B, R)), DIST, R),
        (R + RC, RC, B + RC, ((-RC, RC), (B, R)), DIST, R + RC),
    ]
    for unit in near:
        distances(unit)
    attend(near, False, False)

    n = members * CH
    row_i = lax.broadcasted_iota(jnp.int32, (n, members), 0)
    col_t = lax.broadcasted_iota(jnp.int32, (n, members), 1)
    spread = jnp.where(
        (row_i >= col_t * CH) & (row_i < (col_t + 1) * CH), 1.0, 0.0
    ).astype(BF16)
    half_mix = nn_dot(spread, mix[...]).astype(BF16)
    full_mix = nt_dot(half_mix, spread)
    i2 = lax.broadcasted_iota(jnp.int32, (n, n), 0) & (CH - 1)
    j2 = lax.broadcasted_iota(jnp.int32, (n, n), 1) & (CH - 1)
    KR[...] = jnp.where(i2 == j2, full_mix, 0.0).astype(BF16)

    far_mid = [
        (RC, RC, 2 * B + RC, ((-B + RC, RC),), DMID, 0),
        (R, RC, 2 * B + R, ((B + R, RC),), DMID, RC),
    ]
    far_out = [
        (0, RC, 2 * B, ((-B, R),), DOUT, 0),
        (R + RC, RC, 2 * B + R, ((B + R, R),), DOUT, RC),
    ]
    for unit in far_mid + far_out:
        distances(unit)

    def rows_of(group, core):
        return (RC + core * RC) if group == 0 else core * (R + RC)

    def spread_copy(group, j):
        p, pg, pc = member(j)
        row = pl.multiple_of(rows_of(group, pc) + pg * CH, CH)
        return pltpu.make_async_remote_copy(
            src_ref=BR.at[pl.ds(row, CH)],
            dst_ref=RX.at[group, pl.ds(pl.multiple_of(mine * CH, CH), CH)],
            send_sem=a1s.at[group, j], recv_sem=a1r.at[group, mine],
            device_id={"tm": chip * 2 + pc, "series": pg}, device_id_type=MESH,
        )

    def spread_arrived(group, j):
        p, pg, pc = member(j)
        pltpu.make_async_remote_copy(
            src_ref=BR.at[pl.ds(0, CH)],
            dst_ref=RX.at[group, pl.ds(pl.multiple_of(p * CH, CH), CH)],
            send_sem=a1s.at[group, j], recv_sem=a1r.at[group, p],
            device_id={"tm": chip * 2 + pc, "series": pg}, device_id_type=MESH,
        ).wait_recv()

    def local_rows(group, core):
        return rows_of(group, core) - core * R

    def back_copy(group, j):
        pg = lax.rem(g + j, groups)
        row = pl.multiple_of(local_rows(group, c) + g * CH, CH)
        return pltpu.make_async_remote_copy(
            src_ref=CB.at[group, pl.ds(2 * pg, 2)],
            dst_ref=mix_out.at[:, pl.ds(row, CH), :],
            send_sem=a2s.at[group, j], recv_sem=a2r.at[group, g],
            device_id={"series": pg}, device_id_type=MESH,
        )

    def back_arrived(group, j):
        pg = lax.rem(g + j, groups)
        row = pl.multiple_of(local_rows(group, c) + pg * CH, CH)
        pltpu.make_async_remote_copy(
            src_ref=CB.at[group, pl.ds(0, 2)],
            dst_ref=mix_out.at[:, pl.ds(row, CH), :],
            send_sem=a2s.at[group, j], recv_sem=a2r.at[group, pg],
            device_id={"series": pg}, device_id_type=MESH,
        ).wait_recv()

    def hidden_copy(group):
        src = pl.multiple_of(rows_of(group, other), RC)
        dst = pl.multiple_of(local_rows(group, other), RC)
        return pltpu.make_async_remote_copy(
            src_ref=HID.at[pl.ds(src, RC)], dst_ref=hid_out.at[c, pl.ds(dst, RC)],
            send_sem=hs_sem.at[group, 0], recv_sem=hs_sem.at[group, 1],
            device_id={"tm": sib}, device_id_type=MESH,
        )

    def hidden_keep(group):
        src = pl.multiple_of(rows_of(group, c), RC)
        dst = pl.multiple_of(local_rows(group, c), RC)
        return pltpu.make_async_copy(
            HID.at[pl.ds(src, RC)], hid_out.at[c, pl.ds(dst, RC)], loc_sem.at[4 + group]
        )

    def mixed_keep(group):
        row = pl.multiple_of(local_rows(group, c) + g * CH, CH)
        return pltpu.make_async_copy(
            CB.at[group, pl.ds(2 * g, 2)], mix_out.at[:, pl.ds(row, CH), :], loc_sem.at[6 + group]
        )

    def finish_rows(group, rows):
        @pl.loop(0, D // tile)
        def _(j):
            cols = pl.ds(pl.multiple_of(j * tile, tile), tile)
            own_x = stacked(X, rows, cols)
            update = nn_dot(stacked(ATT, rows), wo[:, cols])
            scatter(HID, rows, cols, (own_x.astype(F32) + update).astype(BF16))

        hidden_copy(group).start()
        hidden_keep(group).start()

        @pl.loop(0, C // tile)
        def _(j):
            cols = pl.ds(pl.multiple_of(j * tile, tile), tile)
            scatter(BR, rows, cols, nn_dot(stacked(HID, rows), wd[:, cols]).astype(BF16))

        for j in range(1, members):
            spread_copy(group, j).start()
        row = pl.multiple_of(rows_of(group, c) + g * CH, CH)
        RX[group, pl.ds(pl.multiple_of(mine * CH, CH), CH), :] = BR[pl.ds(row, CH), :]

    def mix_rows(group):
        for j in range(1, members):
            spread_arrived(group, j)
        CB[group] = nn_dot(KR[...], RX[group]).astype(BF16).reshape(members, CH, C)
        for j in range(1, groups):
            back_copy(group, j).start()
        mixed_keep(group).start()

    mid_rows = [(RC, R)]
    out_rows = [(0, RC), (R + RC, RC)]
    halo_arrived(1, 0)
    project([(2 * B + RC, R)], False)
    attend(far_mid, False, True)
    loads[1].wait()
    loads[2].wait()
    finish_rows(0, mid_rows)
    halo_arrived(1, 1)
    project([(halo_row(1, 0, 1), RC), (halo_row(1, 1, 1), RC)], False)
    attend(far_out, False, True)
    finish_rows(1, out_rows)
    mix_rows(0)
    mix_rows(1)
    for group in range(2):
        hidden_copy(group).wait_recv()
        hidden_keep(group).wait()
        mixed_keep(group).wait()
        for j in range(1, groups):
            back_arrived(group, j)

    sib_copy.wait_send()
    halo_sent(0, 1)
    for k in range(2):
        halo_sent(1, k)
    for group in range(2):
        hidden_copy(group).wait_send()
        for j in range(1, members):
            spread_copy(group, j).wait_send()
        for j in range(1, groups):
            back_copy(group, j).wait_send()


def on_device(
    history, lengths, head_window, input_proj, output_proj, mixer_down, mixer_up, series_mix
):
    S, R, D = history.shape
    C = mixer_down.shape[1]
    chips = lax.axis_size("tm") // 2
    groups = lax.axis_size("series")
    members = 2 * groups
    B = 2 * R
    RC = R // 2
    CH = RC // groups
    pairs = D // PAIR
    smem = pl.BlockSpec(memory_space=pltpu.SMEM)
    vmem = pl.BlockSpec(memory_space=pltpu.VMEM)
    hbm = pl.BlockSpec(memory_space=pl.ANY)
    dma = pltpu.SemaphoreType.DMA
    hidden, mixed = pl.pallas_call(
        functools.partial(layer_kernel, (chips, groups)),
        out_shape=(
            jax.ShapeDtypeStruct((S, R, D), BF16), jax.ShapeDtypeStruct((S, R, C), BF16)
        ),
        in_specs=[smem, smem, vmem, hbm, hbm, hbm, hbm],
        out_specs=(hbm, hbm),
        scratch_shapes=[
            pltpu.VMEM((3 * B, D), BF16),
            pltpu.VMEM((B, D), BF16),
            pltpu.VMEM((3 * B, D), BF16),
            pltpu.VMEM((3 * B, 2 * D), BF16),
            pltpu.VMEM((pairs, 2, B, PAIR), F32),
            pltpu.VMEM((B, D), F32),
            pltpu.VMEM((B, D), F32),
            pltpu.VMEM((B, B), jnp.int32),
            pltpu.VMEM((R, RC), jnp.int32),
            pltpu.VMEM((R, R), jnp.int32),
            pltpu.VMEM((B, B), F32),
            pltpu.VMEM((B, B), F32),
            pltpu.VMEM((B, PAIR), F32),
            pltpu.VMEM((B, PAIR), F32),
            pltpu.VMEM((B, D), BF16),
            pltpu.VMEM((B, D), BF16),
            pltpu.VMEM((B, C), BF16),
            pltpu.VMEM((2, members * CH, C), BF16),
            pltpu.VMEM((members * CH, members * CH), BF16),
            pltpu.VMEM((2, members, CH, C), BF16),
            pltpu.VMEM(input_proj.shape, BF16),
            pltpu.VMEM(output_proj.shape, BF16),
            pltpu.VMEM(mixer_down.shape, BF16),
            dma((8,)), dma((2,)), dma((2, 2)), dma((2, 2, 2)), dma((2, 2, 2)),
            dma((2, members)), dma((2, members)), dma((2, groups)), dma((2, groups)),
        ],
        compiler_params=pltpu.CompilerParams(
            collective_id=0, has_side_effects=True, vmem_limit_bytes=64 * 1024 * 1024 - 65536
        ),
        name="layer",
    )(lengths, head_window, series_mix, history, input_proj, output_proj, mixer_down)
    update = jnp.einsum("spc,cd->spd", mixed, mixer_up, preferred_element_type=F32)
    return (hidden.astype(F32) + update).astype(BF16)


def solution(mesh):
    in_specs = (P("series", "tm", None), P("series"), P(), P(), P(), P(), P(), P())
    out_specs = P("series", "tm", None)
    return jax.shard_map(
        on_device, mesh=mesh, in_specs=in_specs, out_specs=out_specs, check_vma=False
    )
```

```python
import functools
import math

import jax
import jax.numpy as jnp
from jax import lax
from jax.experimental import pallas as pl
from jax.experimental.pallas import tpu as pltpu
from jax.sharding import PartitionSpec as P

HEAD_SIZE = 64
PAIR = 2 * HEAD_SIZE
NEG = -1e30
FAR = 1 << 20
MESH = pl.DeviceIdType.MESH
BF16 = jnp.bfloat16
F32 = jnp.float32
SCALE = HEAD_SIZE ** -0.5 * math.log2(math.e)


def nt_dot(a, b):
    return lax.dot_general(a, b, (((1,), (1,)), ((), ())), preferred_element_type=F32)


def nn_dot(a, b):
    return jnp.dot(a, b, preferred_element_type=F32)


def layer_kernel(
    dims, lengths, window, mix, hist, wi_any, wo_any, wd_any, hid_out, mix_out,
    X, Q, K, VO, M, L, ACC, DIST, DNO, DMID, DOUT, S0, S1, T0, T1, ATT, HID, BR, RX, KR, CB,
    wi, wo, wd,
    loc_sem, sib_sem, hs_sem, rs_sem, rr_sem, a1s, a1r, a2s, a2r,
):
    chips, groups = dims
    members = 2 * groups
    _, R, D = hist.shape
    B = 2 * R
    RC = R // 2
    C = BR.shape[1]
    CH = RC // groups
    pairs = D // PAIR
    me = lax.axis_index("tm")
    g = lax.axis_index("series")
    c = lax.rem(me, 2)
    chip = me // 2
    other = 1 - c
    sib = chip * 2 + other
    mine = g * 2 + c
    rchip = lax.rem(chip + 1, chips)
    lchip = lax.rem(chip + chips - 1, chips)
    total = chips * B
    has_left = chip > 0
    has_right = chip < chips - 1

    def member(j):
        p = lax.rem(mine + j, members)
        return p, p // 2, lax.rem(p, 2)

    barrier = pltpu.get_barrier_semaphore()
    for nchip in (lchip, rchip):
        for core in range(2):
            pl.semaphore_signal(
                barrier, inc=1, device_id={"tm": nchip * 2 + core}, device_id_type=MESH
            )
    for j in range(1, members):
        _, pg, pc = member(j)
        pl.semaphore_signal(
            barrier, inc=1, device_id={"tm": chip * 2 + pc, "series": pg}, device_id_type=MESH
        )
    own_rows = pl.multiple_of(c * R, R)
    own_load = pltpu.make_async_copy(hist.at[c], X.at[pl.ds(own_rows, R)], loc_sem.at[0])
    own_load.start()
    loads = [
        pltpu.make_async_copy(src, dst, loc_sem.at[1 + i])
        for i, (src, dst) in enumerate(((wi_any, wi), (wo_any, wo), (wd_any, wd)))
    ]
    loads[0].start()
    pl.semaphore_wait(barrier, 4 + members - 1)

    sib_copy = pltpu.make_async_remote_copy(
        src_ref=hist.at[other], dst_ref=X.at[pl.ds(own_rows, R)],
        send_sem=sib_sem.at[0], recv_sem=sib_sem.at[1],
        device_id={"tm": sib}, device_id_type=MESH,
    )
    sib_copy.start()

    sends = (
        jnp.where(c == 1, has_right, has_left),
        jnp.where(c == 1, has_left, has_right),
    )

    def halo_copy(phase, k, s):
        if phase == 0:
            target = jnp.where(c == 1, rchip, lchip)
            side = 1 - c
            kk = k + c * (1 - 2 * k)
            base = B + side * R
        else:
            target = jnp.where(c == 1, lchip, rchip)
            side = c
            kk = (1 - k) + c * (2 * k - 1)
            base = 2 * B + side * R
        row = pl.multiple_of(base + kk * RC, RC)
        return pltpu.make_async_remote_copy(
            src_ref=hist.at[s, pl.ds(pl.multiple_of(kk * RC, RC), RC)],
            dst_ref=X.at[pl.ds(row, RC)],
            send_sem=rs_sem.at[phase, k, s], recv_sem=rr_sem.at[phase, side, k],
            device_id={"tm": target * 2 + s}, device_id_type=MESH,
        )

    def halo_row(phase, side, k):
        return (phase + 1) * B + side * R + ((1 - k) if side == 0 else k) * RC

    def halo_arrived(phase, k):
        for side in range(2):
            @pl.when((has_left, has_right)[side])
            def _():
                pltpu.make_async_remote_copy(
                    src_ref=hist.at[0, pl.ds(0, RC)],
                    dst_ref=X.at[pl.ds(halo_row(phase, side, k), RC)],
                    send_sem=rs_sem.at[phase, k, 0], recv_sem=rr_sem.at[phase, side, k],
                    device_id={"tm": sib}, device_id_type=MESH,
                ).wait_recv()

    def start_halo(phase):
        @pl.when(sends[phase])
        def _():
            for k in range(2):
                for s in range(2):
                    halo_copy(phase, k, s).start()

    def halo_sent(phase, k):
        @pl.when(sends[phase])
        def _():
            for s in range(2):
                halo_copy(phase, k, s).wait_send()

    start_halo(0)
    for load in loads[1:]:
        load.start()

    @pl.when(jnp.logical_not(has_left))
    def _():
        for phase in range(1, 3):
            X[phase * B:phase * B + R, :] = jnp.zeros((R, D), BF16)

    @pl.when(jnp.logical_not(has_right))
    def _():
        for phase in range(1, 3):
            X[phase * B + R:(phase + 1) * B, :] = jnp.zeros((R, D), BF16)

    for p in range(pairs):
        VO[:, p * 2 * PAIR + PAIR:(p + 1) * 2 * PAIR] = jnp.ones((3 * B, PAIR), BF16)

    tile = 256

    def stacked(ref, rows, cols=slice(None)):
        parts = [ref[pl.ds(first, count), cols] for first, count in rows]
        return parts[0] if len(parts) == 1 else jnp.concatenate(parts, axis=0)

    def scatter(ref, rows, cols, value):
        at = 0
        for first, count in rows:
            ref[pl.ds(first, count), cols] = value[at:at + count]
            at += count

    def project(rows, with_queries):
        @pl.loop(0, D // tile)
        def _(j):
            cols = pl.ds(pl.multiple_of(j * tile, tile), tile)
            x = stacked(X, rows)
            if with_queries:
                scatter(Q, rows, cols, (nn_dot(x, wi[:, cols]) * SCALE).astype(BF16))
            kcols = pl.ds(pl.multiple_of(D + j * tile, tile), tile)
            scatter(K, rows, cols, nn_dot(x, wi[:, kcols]).astype(BF16))
            wcols = pl.ds(pl.multiple_of(2 * D + j * tile, tile), tile)
            values = nn_dot(x, wi[:, wcols]).astype(BF16)
            for i in range(tile // PAIR):
                at = pl.multiple_of((j * (tile // PAIR) + i) * 2 * PAIR, 2 * PAIR)
                scatter(VO, rows, pl.ds(at, PAIR), values[:, i * PAIR:(i + 1) * PAIR])

    length = lengths[c]
    first_valid = total - length

    def distances(unit):
        q_first, n, _, segments, ref, at = unit
        column = 0
        for k_first, k_count in segments:
            qi = q_first + lax.broadcasted_iota(jnp.int32, (n, k_count), 0)
            kj = k_first + lax.broadcasted_iota(jnp.int32, (n, k_count), 1)
            kpos = chip * B + kj
            valid = (kpos >= first_valid) & (kpos < total) & (kpos >= 0)
            ref[at:at + n, column:column + k_count] = jnp.where(valid, jnp.abs(qi - kj), FAR)
            column += k_count

    def pair_cols(hp):
        return pl.ds(pl.multiple_of(hp * PAIR, PAIR), PAIR)

    def scores(unit, hp, S, T, r0=0):
        q_first, n, ranges, _, ref, at = unit
        count = sum(k_count for _, k_count in ranges)
        low = lax.broadcasted_iota(jnp.int32, (n, PAIR), 1) < HEAD_SIZE
        cols = pair_cols(hp)
        q = Q[q_first:q_first + n, cols]
        zero = jnp.zeros_like(q)
        both = jnp.concatenate([jnp.where(low, q, zero), jnp.where(low, zero, q)], axis=0)
        parts = [nt_dot(both, K[k_row:k_row + k_count, cols]) for k_row, k_count in ranges]
        s = parts[0] if len(parts) == 1 else jnp.concatenate(parts, axis=1)
        dist = ref[at:at + n, :count]
        s = jnp.concatenate([
            jnp.where(dist <= window[2 * hp], s[:n], NEG),
            jnp.where(dist <= window[2 * hp + 1], s[n:], NEG),
        ], axis=0)
        S[r0:r0 + 2 * n, :count] = s
        top = jnp.max(s, axis=1, keepdims=True)
        T[r0:r0 + 2 * n, :] = jnp.broadcast_to(top, (2 * n, PAIR))

    def values(unit, hp, S, T, first, last, r0=0):
        q_first, n, ranges, _, _, _ = unit
        count = sum(k_count for _, k_count in ranges)
        low = lax.broadcasted_iota(jnp.int32, (n, PAIR), 1) < HEAD_SIZE
        cols = pair_cols(hp)
        vcols = pl.ds(pl.multiple_of(hp * 2 * PAIR, 2 * PAIR), 2 * PAIR)
        q_rows = slice(q_first, q_first + n)
        top = T[r0:r0 + 2 * n, :]
        if not first:
            old = jnp.concatenate([M[hp, 0, q_rows, :], M[hp, 1, q_rows, :]], axis=0)
            top = jnp.maximum(top, old)
        added = None
        column = 0
        for k_row, k_count in ranges:
            step = min(PAIR, k_count)
            p = jnp.concatenate([
                jnp.exp2(S[r0:r0 + 2 * n, i:i + step] - top[:, :step]).astype(BF16)
                for i in range(column, column + k_count, step)
            ], axis=1)
            part = nn_dot(p, VO[k_row:k_row + k_count, vcols])
            added = part if added is None else added + part
            column += k_count
        acc = jnp.where(low, added[:n, :PAIR], added[n:, :PAIR])
        sums = jnp.where(low, added[:n, PAIR:], added[n:, PAIR:])
        if not first:
            alpha = jnp.exp2(jnp.where(low, old[:n] - top[:n], old[n:] - top[n:]))
            acc = acc + ACC[q_rows, cols] * alpha
            sums = sums + L[q_rows, cols] * alpha
        if last:
            qpos = chip * B + q_first + lax.broadcasted_iota(jnp.int32, (n, PAIR), 0)
            ATT[q_rows, cols] = jnp.where(qpos >= first_valid, acc / sums, 0.0).astype(BF16)
        else:
            M[hp, 0, q_rows, :] = top[:n]
            M[hp, 1, q_rows, :] = top[n:]
            ACC[q_rows, cols] = acc
            L[q_rows, cols] = sums

    def attend(units, first, last):
        if units[0][1] == R:
            batches = [[(units[0], 0, 0)], [(units[1], 0, 0)]]
            step = 1
        else:
            batches = [[(unit, i, 2 * RC * b) for b, unit in enumerate(units)] for i in range(2)]
            step = 2

        def all_scores(batch, hp, S, T):
            for unit, plus, r0 in batch:
                scores(unit, hp + plus, S, T, r0)

        def all_values(batch, hp, S, T):
            for unit, plus, r0 in batch:
                values(unit, hp + plus, S, T, first, last, r0)

        all_scores(batches[0], 0, S0, T0)

        @pl.loop(0, pairs // step)
        def _(i):
            hp = i * step
            all_scores(batches[1], hp, S1, T1)
            all_values(batches[0], hp, S0, T0)
            all_scores(batches[0], jnp.minimum(hp + step, pairs - step), S0, T0)
            all_values(batches[1], hp, S1, T1)

    own = [(b * R, R, ((0, B),), ((0, B),), DIST, b * R) for b in range(2)]
    near_out = [
        (0, RC, ((B, B - RC),), ((-R, R), (B, RC)), DNO, 0),
        (R + RC, RC, ((B + RC, B - RC),), ((-RC, RC), (B, R)), DNO, RC),
    ]
    near_segments = ((-R, R), (B, R))
    mid = [
        (RC, RC, ((B, B), (2 * B + RC, RC)), near_segments + ((-B + RC, RC),), DMID, 0),
        (R, RC, ((B, B), (2 * B + R, RC)), near_segments + ((B + R, RC),), DMID, RC),
    ]
    far_out = [
        (0, RC, ((2 * B, R),), ((-B, R),), DOUT, 0),
        (R + RC, RC, ((2 * B + R, R),), ((B + R, R),), DOUT, RC),
    ]

    own_load.wait()
    loads[0].wait()
    project([(own_rows, R)], True)
    sib_copy.wait_recv()
    project([(pl.multiple_of(other * R, R), R)], True)
    halo_sent(0, 0)
    start_halo(1)
    for unit in own:
        distances(unit)
    attend(own, True, False)
    for unit in near_out + mid + far_out:
        distances(unit)

    n = members * CH
    row_i = lax.broadcasted_iota(jnp.int32, (n, members), 0)
    col_t = lax.broadcasted_iota(jnp.int32, (n, members), 1)
    spread = jnp.where(
        (row_i >= col_t * CH) & (row_i < (col_t + 1) * CH), 1.0, 0.0
    ).astype(BF16)
    half_mix = nn_dot(spread, mix[...]).astype(BF16)
    full_mix = nt_dot(half_mix, spread)
    i2 = lax.broadcasted_iota(jnp.int32, (n, n), 0) & (CH - 1)
    j2 = lax.broadcasted_iota(jnp.int32, (n, n), 1) & (CH - 1)
    KR[...] = jnp.where(i2 == j2, full_mix, 0.0).astype(BF16)

    def rows_of(group, core):
        return (RC + core * RC) if group == 0 else core * (R + RC)

    def spread_copy(group, j):
        p, pg, pc = member(j)
        row = pl.multiple_of(rows_of(group, pc) + pg * CH, CH)
        return pltpu.make_async_remote_copy(
            src_ref=BR.at[pl.ds(row, CH)],
            dst_ref=RX.at[group, pl.ds(pl.multiple_of(mine * CH, CH), CH)],
            send_sem=a1s.at[group, j], recv_sem=a1r.at[group, mine],
            device_id={"tm": chip * 2 + pc, "series": pg}, device_id_type=MESH,
        )

    def spread_arrived(group, j):
        p, pg, pc = member(j)
        pltpu.make_async_remote_copy(
            src_ref=BR.at[pl.ds(0, CH)],
            dst_ref=RX.at[group, pl.ds(pl.multiple_of(p * CH, CH), CH)],
            send_sem=a1s.at[group, j], recv_sem=a1r.at[group, p],
            device_id={"tm": chip * 2 + pc, "series": pg}, device_id_type=MESH,
        ).wait_recv()

    def local_rows(group, core):
        return rows_of(group, core) - core * R

    def back_copy(group, j):
        pg = lax.rem(g + j, groups)
        row = pl.multiple_of(local_rows(group, c) + g * CH, CH)
        return pltpu.make_async_remote_copy(
            src_ref=CB.at[group, pl.ds(2 * pg, 2)],
            dst_ref=mix_out.at[:, pl.ds(row, CH), :],
            send_sem=a2s.at[group, j], recv_sem=a2r.at[group, g],
            device_id={"series": pg}, device_id_type=MESH,
        )

    def back_arrived(group, j):
        pg = lax.rem(g + j, groups)
        row = pl.multiple_of(local_rows(group, c) + pg * CH, CH)
        pltpu.make_async_remote_copy(
            src_ref=CB.at[group, pl.ds(0, 2)],
            dst_ref=mix_out.at[:, pl.ds(row, CH), :],
            send_sem=a2s.at[group, j], recv_sem=a2r.at[group, pg],
            device_id={"series": pg}, device_id_type=MESH,
        ).wait_recv()

    def hidden_copy(group):
        src = pl.multiple_of(rows_of(group, other), RC)
        dst = pl.multiple_of(local_rows(group, other), RC)
        return pltpu.make_async_remote_copy(
            src_ref=HID.at[pl.ds(src, RC)], dst_ref=hid_out.at[c, pl.ds(dst, RC)],
            send_sem=hs_sem.at[group, 0], recv_sem=hs_sem.at[group, 1],
            device_id={"tm": sib}, device_id_type=MESH,
        )

    def hidden_keep(group):
        src = pl.multiple_of(rows_of(group, c), RC)
        dst = pl.multiple_of(local_rows(group, c), RC)
        return pltpu.make_async_copy(
            HID.at[pl.ds(src, RC)], hid_out.at[c, pl.ds(dst, RC)], loc_sem.at[4 + group]
        )

    def mixed_keep(group):
        row = pl.multiple_of(local_rows(group, c) + g * CH, CH)
        return pltpu.make_async_copy(
            CB.at[group, pl.ds(2 * g, 2)], mix_out.at[:, pl.ds(row, CH), :], loc_sem.at[6 + group]
        )

    def finish_rows(group, rows):
        @pl.loop(0, D // tile)
        def _(j):
            cols = pl.ds(pl.multiple_of(j * tile, tile), tile)
            own_x = stacked(X, rows, cols)
            update = nn_dot(stacked(ATT, rows), wo[:, cols])
            scatter(HID, rows, cols, (own_x.astype(F32) + update).astype(BF16))

        hidden_copy(group).start()
        hidden_keep(group).start()

        @pl.loop(0, C // tile)
        def _(j):
            cols = pl.ds(pl.multiple_of(j * tile, tile), tile)
            scatter(BR, rows, cols, nn_dot(stacked(HID, rows), wd[:, cols]).astype(BF16))

        for j in range(1, members):
            spread_copy(group, j).start()
        row = pl.multiple_of(rows_of(group, c) + g * CH, CH)
        RX[group, pl.ds(pl.multiple_of(mine * CH, CH), CH), :] = BR[pl.ds(row, CH), :]

    def mix_rows(group):
        for j in range(1, members):
            spread_arrived(group, j)
        CB[group] = nn_dot(KR[...], RX[group]).astype(BF16).reshape(members, CH, C)
        for j in range(1, groups):
            back_copy(group, j).start()
        mixed_keep(group).start()

    mid_rows = [(RC, R)]
    out_rows = [(0, RC), (R + RC, RC)]
    for k in range(2):
        halo_arrived(0, k)
    project([(B, B)], False)
    attend(near_out, False, False)
    halo_arrived(1, 0)
    project([(2 * B + RC, R)], False)
    attend(mid, False, True)
    loads[1].wait()
    loads[2].wait()
    finish_rows(0, mid_rows)
    halo_arrived(1, 1)
    project([(halo_row(1, 0, 1), RC), (halo_row(1, 1, 1), RC)], False)
    attend(far_out, False, True)
    finish_rows(1, out_rows)
    mix_rows(0)
    mix_rows(1)
    for group in range(2):
        hidden_copy(group).wait_recv()
        hidden_keep(group).wait()
        mixed_keep(group).wait()
        for j in range(1, groups):
            back_arrived(group, j)

    sib_copy.wait_send()
    halo_sent(0, 1)
    for k in range(2):
        halo_sent(1, k)
    for group in range(2):
        hidden_copy(group).wait_send()
        for j in range(1, members):
            spread_copy(group, j).wait_send()
        for j in range(1, groups):
            back_copy(group, j).wait_send()


def put_kernel(hidden, mixed, wu, out):
    out[...] = (hidden[...].astype(F32) + nn_dot(mixed[...], wu[...])).astype(BF16)


def on_device(
    history, lengths, head_window, input_proj, output_proj, mixer_down, mixer_up, series_mix
):
    S, R, D = history.shape
    C = mixer_down.shape[1]
    chips = lax.axis_size("tm") // 2
    groups = lax.axis_size("series")
    members = 2 * groups
    B = 2 * R
    RC = R // 2
    CH = RC // groups
    pairs = D // PAIR
    smem = pl.BlockSpec(memory_space=pltpu.SMEM)
    vmem = pl.BlockSpec(memory_space=pltpu.VMEM)
    hbm = pl.BlockSpec(memory_space=pl.ANY)
    dma = pltpu.SemaphoreType.DMA
    hidden, mixed = pl.pallas_call(
        functools.partial(layer_kernel, (chips, groups)),
        out_shape=(
            jax.ShapeDtypeStruct((S, R, D), BF16), jax.ShapeDtypeStruct((S, R, C), BF16)
        ),
        in_specs=[smem, smem, vmem, hbm, hbm, hbm, hbm],
        out_specs=(hbm, hbm),
        scratch_shapes=[
            pltpu.VMEM((3 * B, D), BF16),
            pltpu.VMEM((B, D), BF16),
            pltpu.VMEM((3 * B, D), BF16),
            pltpu.VMEM((3 * B, 2 * D), BF16),
            pltpu.VMEM((pairs, 2, B, PAIR), F32),
            pltpu.VMEM((B, D), F32),
            pltpu.VMEM((B, D), F32),
            pltpu.VMEM((B, B), jnp.int32),
            pltpu.VMEM((R, B - RC), jnp.int32),
            pltpu.VMEM((R, B + RC), jnp.int32),
            pltpu.VMEM((R, R), jnp.int32),
            pltpu.VMEM((B, B + RC), F32),
            pltpu.VMEM((B, B + RC), F32),
            pltpu.VMEM((B, PAIR), F32),
            pltpu.VMEM((B, PAIR), F32),
            pltpu.VMEM((B, D), BF16),
            pltpu.VMEM((B, D), BF16),
            pltpu.VMEM((B, C), BF16),
            pltpu.VMEM((2, members * CH, C), BF16),
            pltpu.VMEM((members * CH, members * CH), BF16),
            pltpu.VMEM((2, members, CH, C), BF16),
            pltpu.VMEM(input_proj.shape, BF16),
            pltpu.VMEM(output_proj.shape, BF16),
            pltpu.VMEM(mixer_down.shape, BF16),
            dma((8,)), dma((2,)), dma((2, 2)), dma((2, 2, 2)), dma((2, 2, 2)),
            dma((2, members)), dma((2, members)), dma((2, groups)), dma((2, groups)),
        ],
        compiler_params=pltpu.CompilerParams(
            collective_id=0, has_side_effects=True, vmem_limit_bytes=64 * 1024 * 1024 - 65536
        ),
        name="layer",
    )(lengths, head_window, series_mix, history, input_proj, output_proj, mixer_down)
    rows = S * R
    block = rows // 4
    layer_out = pl.pallas_call(
        put_kernel,
        grid=(4,),
        out_shape=jax.ShapeDtypeStruct((rows, D), BF16),
        in_specs=[
            pl.BlockSpec((block, D), lambda i: (i, 0)),
            pl.BlockSpec((block, C), lambda i: (i, 0)),
            pl.BlockSpec((C, D), lambda i: (0, 0)),
        ],
        out_specs=pl.BlockSpec((block, D), lambda i: (i, 0)),
        name="put",
    )(hidden.reshape(rows, D), mixed.reshape(rows, C), mixer_up)
    return layer_out.reshape(S, R, D)


def solution(mesh):
    in_specs = (P("series", "tm", None), P("series"), P(), P(), P(), P(), P(), P())
    out_specs = P("series", "tm", None)
    return jax.shard_map(
        on_device, mesh=mesh, in_specs=in_specs, out_specs=out_specs, check_vma=False
    )
```

```python
import functools
import math

import jax
import jax.numpy as jnp
from jax import lax
from jax.experimental import pallas as pl
from jax.experimental.pallas import tpu as pltpu
from jax.sharding import PartitionSpec as P

HEAD_SIZE = 64
PAIR = 2 * HEAD_SIZE
NEG = -1e30
FAR = 1 << 20
MESH = pl.DeviceIdType.MESH
BF16 = jnp.bfloat16
F32 = jnp.float32
SCALE = HEAD_SIZE ** -0.5 * math.log2(math.e)


def nt_dot(a, b):
    return lax.dot_general(a, b, (((1,), (1,)), ((), ())), preferred_element_type=F32)


def nn_dot(a, b):
    return jnp.dot(a, b, preferred_element_type=F32)


def layer_kernel(
    dims, lengths, window, mix, hist, wi_any, wo_any, wd_any, hid_out, mix_out,
    X, Q, K, VO, M, L, ACC, DIST, DNO, DMID, DOUT, S0, S1, T0, T1, ATT, HID, BR, RX, KR, CB,
    wi, wo, wd,
    loc_sem, sib_sem, hs_sem, rs_sem, rr_sem, a1s, a1r, a2s, a2r,
):
    chips, groups = dims
    members = 2 * groups
    _, R, D = hist.shape
    B = 2 * R
    RC = R // 2
    C = BR.shape[1]
    CH = RC // groups
    pairs = D // PAIR
    me = lax.axis_index("tm")
    g = lax.axis_index("series")
    c = lax.rem(me, 2)
    chip = me // 2
    other = 1 - c
    sib = chip * 2 + other
    mine = g * 2 + c
    rchip = lax.rem(chip + 1, chips)
    lchip = lax.rem(chip + chips - 1, chips)
    total = chips * B
    has_left = chip > 0
    has_right = chip < chips - 1

    def member(j):
        p = lax.rem(mine + j, members)
        return p, p // 2, lax.rem(p, 2)

    barrier = pltpu.get_barrier_semaphore()
    for nchip in (lchip, rchip):
        for core in range(2):
            pl.semaphore_signal(
                barrier, inc=1, device_id={"tm": nchip * 2 + core}, device_id_type=MESH
            )
    for j in range(1, members):
        _, pg, pc = member(j)
        pl.semaphore_signal(
            barrier, inc=1, device_id={"tm": chip * 2 + pc, "series": pg}, device_id_type=MESH
        )
    own_rows = pl.multiple_of(c * R, R)
    own_load = pltpu.make_async_copy(hist.at[c], X.at[pl.ds(own_rows, R)], loc_sem.at[0])
    own_load.start()
    loads = [
        pltpu.make_async_copy(src, dst, loc_sem.at[1 + i])
        for i, (src, dst) in enumerate(((wi_any, wi), (wo_any, wo), (wd_any, wd)))
    ]
    loads[0].start()
    pl.semaphore_wait(barrier, 4 + members - 1)

    sib_copy = pltpu.make_async_remote_copy(
        src_ref=hist.at[other], dst_ref=X.at[pl.ds(own_rows, R)],
        send_sem=sib_sem.at[0], recv_sem=sib_sem.at[1],
        device_id={"tm": sib}, device_id_type=MESH,
    )
    sib_copy.start()

    sends = (
        jnp.where(c == 1, has_right, has_left),
        jnp.where(c == 1, has_left, has_right),
    )

    def halo_copy(phase, k, s):
        if phase == 0:
            target = jnp.where(c == 1, rchip, lchip)
            side = 1 - c
            kk = k + c * (1 - 2 * k)
            base = B + side * R
        else:
            target = jnp.where(c == 1, lchip, rchip)
            side = c
            kk = (1 - k) + c * (2 * k - 1)
            base = 2 * B + side * R
        row = pl.multiple_of(base + kk * RC, RC)
        return pltpu.make_async_remote_copy(
            src_ref=hist.at[s, pl.ds(pl.multiple_of(kk * RC, RC), RC)],
            dst_ref=X.at[pl.ds(row, RC)],
            send_sem=rs_sem.at[phase, k, s], recv_sem=rr_sem.at[phase, side, k],
            device_id={"tm": target * 2 + s}, device_id_type=MESH,
        )

    def halo_row(phase, side, k):
        return (phase + 1) * B + side * R + ((1 - k) if side == 0 else k) * RC

    def halo_arrived(phase, k):
        for side in range(2):
            @pl.when((has_left, has_right)[side])
            def _():
                pltpu.make_async_remote_copy(
                    src_ref=hist.at[0, pl.ds(0, RC)],
                    dst_ref=X.at[pl.ds(halo_row(phase, side, k), RC)],
                    send_sem=rs_sem.at[phase, k, 0], recv_sem=rr_sem.at[phase, side, k],
                    device_id={"tm": sib}, device_id_type=MESH,
                ).wait_recv()

    def start_halo(phase):
        @pl.when(sends[phase])
        def _():
            for k in range(2):
                for s in range(2):
                    halo_copy(phase, k, s).start()

    def halo_sent(phase, k):
        @pl.when(sends[phase])
        def _():
            for s in range(2):
                halo_copy(phase, k, s).wait_send()

    start_halo(0)
    for load in loads[1:]:
        load.start()

    @pl.when(jnp.logical_not(has_left))
    def _():
        for phase in range(1, 3):
            X[phase * B:phase * B + R, :] = jnp.zeros((R, D), BF16)

    @pl.when(jnp.logical_not(has_right))
    def _():
        for phase in range(1, 3):
            X[phase * B + R:(phase + 1) * B, :] = jnp.zeros((R, D), BF16)

    for p in range(pairs):
        VO[:, p * 2 * PAIR + PAIR:(p + 1) * 2 * PAIR] = jnp.ones((3 * B, PAIR), BF16)

    tile = 256

    def stacked(ref, rows, cols=slice(None)):
        parts = [ref[pl.ds(first, count), cols] for first, count in rows]
        return parts[0] if len(parts) == 1 else jnp.concatenate(parts, axis=0)

    def scatter(ref, rows, cols, value):
        at = 0
        for first, count in rows:
            ref[pl.ds(first, count), cols] = value[at:at + count]
            at += count

    def project(rows, with_queries):
        @pl.loop(0, D // tile)
        def _(j):
            cols = pl.ds(pl.multiple_of(j * tile, tile), tile)
            x = stacked(X, rows)
            if with_queries:
                scatter(Q, rows, cols, (nn_dot(x, wi[:, cols]) * SCALE).astype(BF16))
            kcols = pl.ds(pl.multiple_of(D + j * tile, tile), tile)
            scatter(K, rows, cols, nn_dot(x, wi[:, kcols]).astype(BF16))
            wcols = pl.ds(pl.multiple_of(2 * D + j * tile, tile), tile)
            values = nn_dot(x, wi[:, wcols]).astype(BF16)
            for i in range(tile // PAIR):
                at = pl.multiple_of((j * (tile // PAIR) + i) * 2 * PAIR, 2 * PAIR)
                scatter(VO, rows, pl.ds(at, PAIR), values[:, i * PAIR:(i + 1) * PAIR])

    length = lengths[c]
    first_valid = total - length

    def distances(unit):
        q_first, n, _, segments, ref, at = unit
        column = 0
        for k_first, k_count in segments:
            qi = q_first + lax.broadcasted_iota(jnp.int32, (n, k_count), 0)
            kj = k_first + lax.broadcasted_iota(jnp.int32, (n, k_count), 1)
            kpos = chip * B + kj
            valid = (kpos >= first_valid) & (kpos < total) & (kpos >= 0)
            ref[at:at + n, column:column + k_count] = jnp.where(valid, jnp.abs(qi - kj), FAR)
            column += k_count

    def pair_cols(hp):
        return pl.ds(pl.multiple_of(hp * PAIR, PAIR), PAIR)

    def scores(unit, hp, S, T, r0=0):
        q_first, n, ranges, _, ref, at = unit
        count = sum(k_count for _, k_count in ranges)
        low = lax.broadcasted_iota(jnp.int32, (n, PAIR), 1) < HEAD_SIZE
        cols = pair_cols(hp)
        q = Q[q_first:q_first + n, cols]
        zero = jnp.zeros_like(q)
        both = jnp.concatenate([jnp.where(low, q, zero), jnp.where(low, zero, q)], axis=0)
        parts = [nt_dot(both, K[k_row:k_row + k_count, cols]) for k_row, k_count in ranges]
        s = parts[0] if len(parts) == 1 else jnp.concatenate(parts, axis=1)
        dist = ref[at:at + n, :count]
        s = jnp.concatenate([
            jnp.where(dist <= window[2 * hp], s[:n], NEG),
            jnp.where(dist <= window[2 * hp + 1], s[n:], NEG),
        ], axis=0)
        S[r0:r0 + 2 * n, :count] = s
        top = jnp.max(s, axis=1, keepdims=True)
        T[r0:r0 + 2 * n, :] = jnp.broadcast_to(top, (2 * n, PAIR))

    def values(unit, hp, S, T, first, last, r0=0):
        q_first, n, ranges, _, _, _ = unit
        count = sum(k_count for _, k_count in ranges)
        low = lax.broadcasted_iota(jnp.int32, (n, PAIR), 1) < HEAD_SIZE
        cols = pair_cols(hp)
        vcols = pl.ds(pl.multiple_of(hp * 2 * PAIR, 2 * PAIR), 2 * PAIR)
        q_rows = slice(q_first, q_first + n)
        top = T[r0:r0 + 2 * n, :]
        if not first:
            old = jnp.concatenate([M[hp, 0, q_rows, :], M[hp, 1, q_rows, :]], axis=0)
            top = jnp.maximum(top, old)
        added = None
        column = 0
        for k_row, k_count in ranges:
            step = min(PAIR, k_count)
            p = jnp.concatenate([
                jnp.exp2(S[r0:r0 + 2 * n, i:i + step] - top[:, :step]).astype(BF16)
                for i in range(column, column + k_count, step)
            ], axis=1)
            part = nn_dot(p, VO[k_row:k_row + k_count, vcols])
            added = part if added is None else added + part
            column += k_count
        acc = jnp.where(low, added[:n, :PAIR], added[n:, :PAIR])
        sums = jnp.where(low, added[:n, PAIR:], added[n:, PAIR:])
        if not first:
            alpha = jnp.exp2(jnp.where(low, old[:n] - top[:n], old[n:] - top[n:]))
            acc = acc + ACC[q_rows, cols] * alpha
            sums = sums + L[q_rows, cols] * alpha
        if last:
            qpos = chip * B + q_first + lax.broadcasted_iota(jnp.int32, (n, PAIR), 0)
            ATT[q_rows, cols] = jnp.where(qpos >= first_valid, acc / sums, 0.0).astype(BF16)
        else:
            M[hp, 0, q_rows, :] = top[:n]
            M[hp, 1, q_rows, :] = top[n:]
            ACC[q_rows, cols] = acc
            L[q_rows, cols] = sums

    def attend(units, first, last):
        if len(units) == 1:
            batches = [[(units[0], 2 * i + b, 2 * RC * b) for b in range(2)] for i in range(2)]
            step = 4
        elif units[0][1] == R:
            batches = [[(units[0], 0, 0)], [(units[1], 0, 0)]]
            step = 1
        else:
            batches = [[(unit, i, 2 * RC * b) for b, unit in enumerate(units)] for i in range(2)]
            step = 2

        def all_scores(batch, hp, S, T):
            for unit, plus, r0 in batch:
                scores(unit, hp + plus, S, T, r0)

        def all_values(batch, hp, S, T):
            for unit, plus, r0 in batch:
                values(unit, hp + plus, S, T, first, last, r0)

        all_scores(batches[0], 0, S0, T0)

        @pl.loop(0, pairs // step)
        def _(i):
            hp = i * step
            all_scores(batches[1], hp, S1, T1)
            all_values(batches[0], hp, S0, T0)
            all_scores(batches[0], jnp.minimum(hp + step, pairs - step), S0, T0)
            all_values(batches[1], hp, S1, T1)

    own = [(b * R, R, ((0, B),), ((0, B),), DIST, b * R) for b in range(2)]
    near_out = [
        (0, RC, ((B, B - RC),), ((-R, R), (B, RC)), DNO, 0),
        (R + RC, RC, ((B + RC, B - RC),), ((-RC, RC), (B, R)), DNO, RC),
    ]
    near_segments = ((-R, R), (B, R))
    mid = [
        (RC, RC, ((B, B), (2 * B + RC, RC)), near_segments + ((-B + RC, RC),), DMID, 0),
        (R, RC, ((B, B), (2 * B + R, RC)), near_segments + ((B + R, RC),), DMID, RC),
    ]
    far_out = [
        (0, RC, ((2 * B, R),), ((-B, R),), DOUT, 0),
        (R + RC, RC, ((2 * B + R, R),), ((B + R, R),), DOUT, RC),
    ]

    own_load.wait()
    loads[0].wait()
    project([(own_rows, R)], True)
    for unit in own + near_out + mid + far_out:
        distances(unit)

    n = members * CH
    row_i = lax.broadcasted_iota(jnp.int32, (n, members), 0)
    col_t = lax.broadcasted_iota(jnp.int32, (n, members), 1)
    spread = jnp.where(
        (row_i >= col_t * CH) & (row_i < (col_t + 1) * CH), 1.0, 0.0
    ).astype(BF16)
    half_mix = nn_dot(spread, mix[...]).astype(BF16)
    full_mix = nt_dot(half_mix, spread)
    i2 = lax.broadcasted_iota(jnp.int32, (n, n), 0) & (CH - 1)
    j2 = lax.broadcasted_iota(jnp.int32, (n, n), 1) & (CH - 1)
    KR[...] = jnp.where(i2 == j2, full_mix, 0.0).astype(BF16)

    sib_copy.wait_recv()
    project([(pl.multiple_of(other * R, R), R)], True)
    halo_sent(0, 0)
    start_halo(1)
    attend(own, True, False)

    def rows_of(group, core):
        return (RC + core * RC) if group == 0 else core * (R + RC)

    def spread_copy(group, j):
        p, pg, pc = member(j)
        row = pl.multiple_of(rows_of(group, pc) + pg * CH, CH)
        return pltpu.make_async_remote_copy(
            src_ref=BR.at[pl.ds(row, CH)],
            dst_ref=RX.at[group, pl.ds(pl.multiple_of(mine * CH, CH), CH)],
            send_sem=a1s.at[group, j], recv_sem=a1r.at[group, mine],
            device_id={"tm": chip * 2 + pc, "series": pg}, device_id_type=MESH,
        )

    def spread_arrived(group, j):
        p, pg, pc = member(j)
        pltpu.make_async_remote_copy(
            src_ref=BR.at[pl.ds(0, CH)],
            dst_ref=RX.at[group, pl.ds(pl.multiple_of(p * CH, CH), CH)],
            send_sem=a1s.at[group, j], recv_sem=a1r.at[group, p],
            device_id={"tm": chip * 2 + pc, "series": pg}, device_id_type=MESH,
        ).wait_recv()

    def local_rows(group, core):
        return rows_of(group, core) - core * R

    def back_copy(group, j):
        pg = lax.rem(g + j, groups)
        row = pl.multiple_of(local_rows(group, c) + g * CH, CH)
        return pltpu.make_async_remote_copy(
            src_ref=CB.at[group, pl.ds(2 * pg, 2)],
            dst_ref=mix_out.at[:, pl.ds(row, CH), :],
            send_sem=a2s.at[group, j], recv_sem=a2r.at[group, g],
            device_id={"series": pg}, device_id_type=MESH,
        )

    def back_arrived(group, j):
        pg = lax.rem(g + j, groups)
        row = pl.multiple_of(local_rows(group, c) + pg * CH, CH)
        pltpu.make_async_remote_copy(
            src_ref=CB.at[group, pl.ds(0, 2)],
            dst_ref=mix_out.at[:, pl.ds(row, CH), :],
            send_sem=a2s.at[group, j], recv_sem=a2r.at[group, pg],
            device_id={"series": pg}, device_id_type=MESH,
        ).wait_recv()

    def hidden_copy(group):
        src = pl.multiple_of(rows_of(group, other), RC)
        dst = pl.multiple_of(local_rows(group, other), RC)
        return pltpu.make_async_remote_copy(
            src_ref=HID.at[pl.ds(src, RC)], dst_ref=hid_out.at[c, pl.ds(dst, RC)],
            send_sem=hs_sem.at[group, 0], recv_sem=hs_sem.at[group, 1],
            device_id={"tm": sib}, device_id_type=MESH,
        )

    def hidden_keep(group):
        src = pl.multiple_of(rows_of(group, c), RC)
        dst = pl.multiple_of(local_rows(group, c), RC)
        return pltpu.make_async_copy(
            HID.at[pl.ds(src, RC)], hid_out.at[c, pl.ds(dst, RC)], loc_sem.at[4 + group]
        )

    def mixed_keep(group):
        row = pl.multiple_of(local_rows(group, c) + g * CH, CH)
        return pltpu.make_async_copy(
            CB.at[group, pl.ds(2 * g, 2)], mix_out.at[:, pl.ds(row, CH), :], loc_sem.at[6 + group]
        )

    def finish_rows(group, rows, cores):
        @pl.loop(0, D // tile)
        def _(j):
            cols = pl.ds(pl.multiple_of(j * tile, tile), tile)
            own_x = stacked(X, rows, cols)
            update = nn_dot(stacked(ATT, rows), wo[:, cols])
            scatter(HID, rows, cols, (own_x.astype(F32) + update).astype(BF16))

        if cores[-1] == 1:
            hidden_copy(group).start()
            hidden_keep(group).start()

        @pl.loop(0, C // tile)
        def _(j):
            cols = pl.ds(pl.multiple_of(j * tile, tile), tile)
            scatter(BR, rows, cols, nn_dot(stacked(HID, rows), wd[:, cols]).astype(BF16))

        for core in cores:
            plus = lax.rem(c + core, 2)

            @pl.when(plus == 0)
            def _():
                row = pl.multiple_of(rows_of(group, c) + g * CH, CH)
                RX[group, pl.ds(pl.multiple_of(mine * CH, CH), CH), :] = BR[pl.ds(row, CH), :]

            @pl.when(plus == 1)
            def _():
                spread_copy(group, 1).start()

            for i in range(1, groups):
                spread_copy(group, 2 * i + plus).start()

    def mix_rows(group):
        for j in range(1, members):
            spread_arrived(group, j)
        CB[group] = nn_dot(KR[...], RX[group]).astype(BF16).reshape(members, CH, C)
        for j in range(1, groups):
            back_copy(group, j).start()
        mixed_keep(group).start()

    mid_rows = [(RC, R)]
    out_rows = [(0, RC), (R + RC, RC)]
    for k in range(2):
        halo_arrived(0, k)
    project([(B, B)], False)
    attend(near_out, False, False)
    halo_arrived(1, 0)
    project([(2 * B + RC, R)], False)
    attend(mid, False, True)
    loads[1].wait()
    loads[2].wait()
    finish_rows(0, mid_rows, (0, 1))
    halo_arrived(1, 1)
    project([(halo_row(1, 0, 1), RC), (halo_row(1, 1, 1), RC)], False)
    for core in range(2):
        attend(far_out[core:core + 1], False, True)
        finish_rows(1, out_rows[core:core + 1], (core,))
    mix_rows(0)
    mix_rows(1)
    for group in range(2):
        hidden_copy(group).wait_recv()
        hidden_keep(group).wait()
        mixed_keep(group).wait()
        for j in range(1, groups):
            back_arrived(group, j)

    sib_copy.wait_send()
    halo_sent(0, 1)
    for k in range(2):
        halo_sent(1, k)
    for group in range(2):
        hidden_copy(group).wait_send()
        for j in range(1, members):
            spread_copy(group, j).wait_send()
        for j in range(1, groups):
            back_copy(group, j).wait_send()


def on_device(
    history, lengths, head_window, input_proj, output_proj, mixer_down, mixer_up, series_mix
):
    S, R, D = history.shape
    C = mixer_down.shape[1]
    chips = lax.axis_size("tm") // 2
    groups = lax.axis_size("series")
    members = 2 * groups
    B = 2 * R
    RC = R // 2
    CH = RC // groups
    pairs = D // PAIR
    smem = pl.BlockSpec(memory_space=pltpu.SMEM)
    vmem = pl.BlockSpec(memory_space=pltpu.VMEM)
    hbm = pl.BlockSpec(memory_space=pl.ANY)
    dma = pltpu.SemaphoreType.DMA
    hidden, mixed = pl.pallas_call(
        functools.partial(layer_kernel, (chips, groups)),
        out_shape=(
            jax.ShapeDtypeStruct((S, R, D), BF16), jax.ShapeDtypeStruct((S, R, C), BF16)
        ),
        in_specs=[smem, smem, vmem, hbm, hbm, hbm, hbm],
        out_specs=(hbm, hbm),
        scratch_shapes=[
            pltpu.VMEM((3 * B, D), BF16),
            pltpu.VMEM((B, D), BF16),
            pltpu.VMEM((3 * B, D), BF16),
            pltpu.VMEM((3 * B, 2 * D), BF16),
            pltpu.VMEM((pairs, 2, B, PAIR), F32),
            pltpu.VMEM((B, D), F32),
            pltpu.VMEM((B, D), F32),
            pltpu.VMEM((B, B), jnp.int32),
            pltpu.VMEM((R, B - RC), jnp.int32),
            pltpu.VMEM((R, B + RC), jnp.int32),
            pltpu.VMEM((R, R), jnp.int32),
            pltpu.VMEM((B, B + RC), F32),
            pltpu.VMEM((B, B + RC), F32),
            pltpu.VMEM((B, PAIR), F32),
            pltpu.VMEM((B, PAIR), F32),
            pltpu.VMEM((B, D), BF16),
            pltpu.VMEM((B, D), BF16),
            pltpu.VMEM((B, C), BF16),
            pltpu.VMEM((2, members * CH, C), BF16),
            pltpu.VMEM((members * CH, members * CH), BF16),
            pltpu.VMEM((2, members, CH, C), BF16),
            pltpu.VMEM(input_proj.shape, BF16),
            pltpu.VMEM(output_proj.shape, BF16),
            pltpu.VMEM(mixer_down.shape, BF16),
            dma((8,)), dma((2,)), dma((2, 2)), dma((2, 2, 2)), dma((2, 2, 2)),
            dma((2, members)), dma((2, members)), dma((2, groups)), dma((2, groups)),
        ],
        compiler_params=pltpu.CompilerParams(
            collective_id=0, has_side_effects=True, vmem_limit_bytes=64 * 1024 * 1024 - 65536
        ),
        name="layer",
    )(lengths, head_window, series_mix, history, input_proj, output_proj, mixer_down)
    update = jnp.einsum("spc,cd->spd", mixed, mixer_up, preferred_element_type=F32)
    return (hidden.astype(F32) + update).astype(BF16)


def solution(mesh):
    in_specs = (P("series", "tm", None), P("series"), P(), P(), P(), P(), P(), P())
    out_specs = P("series", "tm", None)
    return jax.shard_map(
        on_device, mesh=mesh, in_specs=in_specs, out_specs=out_specs, check_vma=False
    )
```

```python
import functools
import math

import jax
import jax.numpy as jnp
from jax import lax
from jax.experimental import pallas as pl
from jax.experimental.pallas import tpu as pltpu
from jax.sharding import PartitionSpec as P

HEAD_SIZE = 64
PAIR = 2 * HEAD_SIZE
NEG = -1e30
FAR = 1 << 20
MESH = pl.DeviceIdType.MESH
BF16 = jnp.bfloat16
F32 = jnp.float32
SCALE = HEAD_SIZE ** -0.5 * math.log2(math.e)


def nt_dot(a, b):
    return lax.dot_general(a, b, (((1,), (1,)), ((), ())), preferred_element_type=F32)


def nn_dot(a, b):
    return jnp.dot(a, b, preferred_element_type=F32)


def layer_kernel(
    dims, lengths, window, mix, hist, wi_any, wo_any, wd_any, hid_out, mix_out,
    X, Q, K, VO, M, L, ACC, DIST, DNO, DMID, DOUT, S0, S1, T0, T1, ATT, HID, BR, RX, KR, CB,
    wi, wo, wd,
    loc_sem, sib_sem, hs_sem, rs_sem, rr_sem, a1s, a1r, a2s, a2r,
):
    chips, groups = dims
    members = 2 * groups
    _, R, D = hist.shape
    B = 2 * R
    RC = R // 2
    C = BR.shape[1]
    CH = RC // groups
    pairs = D // PAIR
    me = lax.axis_index("tm")
    g = lax.axis_index("series")
    c = lax.rem(me, 2)
    chip = me // 2
    other = 1 - c
    sib = chip * 2 + other
    mine = g * 2 + c
    rchip = lax.rem(chip + 1, chips)
    lchip = lax.rem(chip + chips - 1, chips)
    total = chips * B
    has_left = chip > 0
    has_right = chip < chips - 1

    def member(j):
        p = lax.rem(mine + j, members)
        return p, p // 2, lax.rem(p, 2)

    barrier = pltpu.get_barrier_semaphore()
    for nchip in (lchip, rchip):
        for core in range(2):
            pl.semaphore_signal(
                barrier, inc=1, device_id={"tm": nchip * 2 + core}, device_id_type=MESH
            )
    for j in range(1, members):
        _, pg, pc = member(j)
        pl.semaphore_signal(
            barrier, inc=1, device_id={"tm": chip * 2 + pc, "series": pg}, device_id_type=MESH
        )
    own_rows = pl.multiple_of(c * R, R)
    own_load = pltpu.make_async_copy(hist.at[c], X.at[pl.ds(own_rows, R)], loc_sem.at[0])
    own_load.start()
    loads = [
        pltpu.make_async_copy(src, dst, loc_sem.at[1 + i])
        for i, (src, dst) in enumerate(((wi_any, wi), (wo_any, wo), (wd_any, wd)))
    ]
    loads[0].start()
    pl.semaphore_wait(barrier, 4 + members - 1)

    sib_copy = pltpu.make_async_remote_copy(
        src_ref=hist.at[other], dst_ref=X.at[pl.ds(own_rows, R)],
        send_sem=sib_sem.at[0], recv_sem=sib_sem.at[1],
        device_id={"tm": sib}, device_id_type=MESH,
    )
    sib_copy.start()

    sends = (
        jnp.where(c == 1, has_right, has_left),
        jnp.where(c == 1, has_left, has_right),
    )

    def halo_copy(phase, k, s):
        if phase == 0:
            target = jnp.where(c == 1, rchip, lchip)
            side = 1 - c
            kk = k + c * (1 - 2 * k)
            base = B + side * R
        else:
            target = jnp.where(c == 1, lchip, rchip)
            side = c
            kk = (1 - k) + c * (2 * k - 1)
            base = 2 * B + side * R
        row = pl.multiple_of(base + kk * RC, RC)
        return pltpu.make_async_remote_copy(
            src_ref=hist.at[s, pl.ds(pl.multiple_of(kk * RC, RC), RC)],
            dst_ref=X.at[pl.ds(row, RC)],
            send_sem=rs_sem.at[phase, k, s], recv_sem=rr_sem.at[phase, side, k],
            device_id={"tm": target * 2 + s}, device_id_type=MESH,
        )

    def halo_row(phase, side, k):
        return (phase + 1) * B + side * R + ((1 - k) if side == 0 else k) * RC

    def halo_arrived(phase, k):
        for side in range(2):
            @pl.when((has_left, has_right)[side])
            def _():
                pltpu.make_async_remote_copy(
                    src_ref=hist.at[0, pl.ds(0, RC)],
                    dst_ref=X.at[pl.ds(halo_row(phase, side, k), RC)],
                    send_sem=rs_sem.at[phase, k, 0], recv_sem=rr_sem.at[phase, side, k],
                    device_id={"tm": sib}, device_id_type=MESH,
                ).wait_recv()

    def start_halo(phase):
        @pl.when(sends[phase])
        def _():
            for k in range(2):
                for s in range(2):
                    halo_copy(phase, k, s).start()

    def halo_sent(phase, k):
        @pl.when(sends[phase])
        def _():
            for s in range(2):
                halo_copy(phase, k, s).wait_send()

    start_halo(0)
    for load in loads[1:]:
        load.start()

    @pl.when(jnp.logical_not(has_left))
    def _():
        for phase in range(1, 3):
            X[phase * B:phase * B + R, :] = jnp.zeros((R, D), BF16)

    @pl.when(jnp.logical_not(has_right))
    def _():
        for phase in range(1, 3):
            X[phase * B + R:(phase + 1) * B, :] = jnp.zeros((R, D), BF16)

    for p in range(pairs):
        VO[:, p * 2 * PAIR + PAIR:(p + 1) * 2 * PAIR] = jnp.ones((3 * B, PAIR), BF16)

    tile = 256

    def stacked(ref, rows, cols=slice(None)):
        parts = [ref[pl.ds(first, count), cols] for first, count in rows]
        return parts[0] if len(parts) == 1 else jnp.concatenate(parts, axis=0)

    def scatter(ref, rows, cols, value):
        at = 0
        for first, count in rows:
            ref[pl.ds(first, count), cols] = value[at:at + count]
            at += count

    def project(rows, with_queries):
        @pl.loop(0, D // tile)
        def _(j):
            cols = pl.ds(pl.multiple_of(j * tile, tile), tile)
            x = stacked(X, rows)
            if with_queries:
                scatter(Q, rows, cols, (nn_dot(x, wi[:, cols]) * SCALE).astype(BF16))
            kcols = pl.ds(pl.multiple_of(D + j * tile, tile), tile)
            scatter(K, rows, cols, nn_dot(x, wi[:, kcols]).astype(BF16))
            wcols = pl.ds(pl.multiple_of(2 * D + j * tile, tile), tile)
            values = nn_dot(x, wi[:, wcols]).astype(BF16)
            for i in range(tile // PAIR):
                at = pl.multiple_of((j * (tile // PAIR) + i) * 2 * PAIR, 2 * PAIR)
                scatter(VO, rows, pl.ds(at, PAIR), values[:, i * PAIR:(i + 1) * PAIR])

    length = lengths[c]
    first_valid = total - length

    def distances(unit):
        q_first, n, _, segments, ref, at = unit
        column = 0
        for k_first, k_count in segments:
            qi = q_first + lax.broadcasted_iota(jnp.int32, (n, k_count), 0)
            kj = k_first + lax.broadcasted_iota(jnp.int32, (n, k_count), 1)
            kpos = chip * B + kj
            valid = (kpos >= first_valid) & (kpos < total) & (kpos >= 0)
            ref[at:at + n, column:column + k_count] = jnp.where(valid, jnp.abs(qi - kj), FAR)
            column += k_count

    def pair_cols(hp):
        return pl.ds(pl.multiple_of(hp * PAIR, PAIR), PAIR)

    def scores(unit, hp, S, T, r0=0):
        q_first, n, ranges, _, ref, at = unit
        count = sum(k_count for _, k_count in ranges)
        low = lax.broadcasted_iota(jnp.int32, (n, PAIR), 1) < HEAD_SIZE
        cols = pair_cols(hp)
        q = Q[q_first:q_first + n, cols]
        zero = jnp.zeros_like(q)
        both = jnp.concatenate([jnp.where(low, q, zero), jnp.where(low, zero, q)], axis=0)
        parts = [nt_dot(both, K[k_row:k_row + k_count, cols]) for k_row, k_count in ranges]
        s = parts[0] if len(parts) == 1 else jnp.concatenate(parts, axis=1)
        dist = ref[at:at + n, :count]
        s = jnp.concatenate([
            jnp.where(dist <= window[2 * hp], s[:n], NEG),
            jnp.where(dist <= window[2 * hp + 1], s[n:], NEG),
        ], axis=0)
        S[r0:r0 + 2 * n, :count] = s
        lanes = min(PAIR, count)
        T[r0:r0 + 2 * n, :lanes] = functools.reduce(
            jnp.maximum, [s[:, i:i + lanes] for i in range(0, count, lanes)]
        )

    def values(unit, hp, S, T, first, last, r0=0):
        q_first, n, ranges, _, _, _ = unit
        count = sum(k_count for _, k_count in ranges)
        low = lax.broadcasted_iota(jnp.int32, (n, PAIR), 1) < HEAD_SIZE
        cols = pair_cols(hp)
        vcols = pl.ds(pl.multiple_of(hp * 2 * PAIR, 2 * PAIR), 2 * PAIR)
        q_rows = slice(q_first, q_first + n)
        lanes = min(PAIR, count)
        top = jnp.max(T[r0:r0 + 2 * n, :lanes], axis=1, keepdims=True)
        top = jnp.broadcast_to(top, (2 * n, PAIR))
        if not first:
            old = jnp.concatenate([M[hp, 0, q_rows, :], M[hp, 1, q_rows, :]], axis=0)
            top = jnp.maximum(top, old)
        added = None
        column = 0
        for k_row, k_count in ranges:
            step = min(PAIR, k_count)
            p = jnp.concatenate([
                jnp.exp2(S[r0:r0 + 2 * n, i:i + step] - top[:, :step]).astype(BF16)
                for i in range(column, column + k_count, step)
            ], axis=1)
            part = nn_dot(p, VO[k_row:k_row + k_count, vcols])
            added = part if added is None else added + part
            column += k_count
        acc = jnp.where(low, added[:n, :PAIR], added[n:, :PAIR])
        sums = jnp.where(low, added[:n, PAIR:], added[n:, PAIR:])
        if not first:
            alpha = jnp.exp2(jnp.where(low, old[:n] - top[:n], old[n:] - top[n:]))
            acc = acc + ACC[q_rows, cols] * alpha
            sums = sums + L[q_rows, cols] * alpha
        if last:
            qpos = chip * B + q_first + lax.broadcasted_iota(jnp.int32, (n, PAIR), 0)
            ATT[q_rows, cols] = jnp.where(qpos >= first_valid, acc / sums, 0.0).astype(BF16)
        else:
            M[hp, 0, q_rows, :] = top[:n]
            M[hp, 1, q_rows, :] = top[n:]
            ACC[q_rows, cols] = acc
            L[q_rows, cols] = sums

    def attend(units, first, last):
        if len(units) == 1:
            batches = [[(units[0], 2 * i + b, 2 * RC * b) for b in range(2)] for i in range(2)]
            step = 4
        elif units[0][1] == R:
            batches = [[(units[0], 0, 0)], [(units[1], 0, 0)]]
            step = 1
        else:
            batches = [[(unit, i, 2 * RC * b) for b, unit in enumerate(units)] for i in range(2)]
            step = 2

        def all_scores(batch, hp, S, T):
            for unit, plus, r0 in batch:
                scores(unit, hp + plus, S, T, r0)

        def all_values(batch, hp, S, T):
            for unit, plus, r0 in batch:
                values(unit, hp + plus, S, T, first, last, r0)

        all_scores(batches[0], 0, S0, T0)

        @pl.loop(0, pairs // step)
        def _(i):
            hp = i * step
            all_scores(batches[1], hp, S1, T1)
            all_values(batches[0], hp, S0, T0)
            all_scores(batches[0], jnp.minimum(hp + step, pairs - step), S0, T0)
            all_values(batches[1], hp, S1, T1)

    own = [(b * R, R, ((0, B),), ((0, B),), DIST, b * R) for b in range(2)]
    near_out = [
        (0, RC, ((B, B - RC),), ((-R, R), (B, RC)), DNO, 0),
        (R + RC, RC, ((B + RC, B - RC),), ((-RC, RC), (B, R)), DNO, RC),
    ]
    near_segments = ((-R, R), (B, R))
    mid = [
        (RC, RC, ((B, B), (2 * B + RC, RC)), near_segments + ((-B + RC, RC),), DMID, 0),
        (R, RC, ((B, B), (2 * B + R, RC)), near_segments + ((B + R, RC),), DMID, RC),
    ]
    far_out = [
        (0, RC, ((2 * B, R),), ((-B, R),), DOUT, 0),
        (R + RC, RC, ((2 * B + R, R),), ((B + R, R),), DOUT, RC),
    ]

    own_load.wait()
    loads[0].wait()
    project([(own_rows, R)], True)
    for unit in own + near_out + mid + far_out:
        distances(unit)

    n = members * CH
    row_i = lax.broadcasted_iota(jnp.int32, (n, members), 0)
    col_t = lax.broadcasted_iota(jnp.int32, (n, members), 1)
    spread = jnp.where(
        (row_i >= col_t * CH) & (row_i < (col_t + 1) * CH), 1.0, 0.0
    ).astype(BF16)
    half_mix = nn_dot(spread, mix[...]).astype(BF16)
    full_mix = nt_dot(half_mix, spread)
    i2 = lax.broadcasted_iota(jnp.int32, (n, n), 0) & (CH - 1)
    j2 = lax.broadcasted_iota(jnp.int32, (n, n), 1) & (CH - 1)
    KR[...] = jnp.where(i2 == j2, full_mix, 0.0).astype(BF16)

    sib_copy.wait_recv()
    project([(pl.multiple_of(other * R, R), R)], True)
    halo_sent(0, 0)
    start_halo(1)
    attend(own, True, False)

    def rows_of(group, core):
        return (RC + core * RC) if group == 0 else core * (R + RC)

    def spread_copy(group, j):
        p, pg, pc = member(j)
        row = pl.multiple_of(rows_of(group, pc) + pg * CH, CH)
        return pltpu.make_async_remote_copy(
            src_ref=BR.at[pl.ds(row, CH)],
            dst_ref=RX.at[group, pl.ds(pl.multiple_of(mine * CH, CH), CH)],
            send_sem=a1s.at[group, j], recv_sem=a1r.at[group, mine],
            device_id={"tm": chip * 2 + pc, "series": pg}, device_id_type=MESH,
        )

    def spread_arrived(group, j):
        p, pg, pc = member(j)
        pltpu.make_async_remote_copy(
            src_ref=BR.at[pl.ds(0, CH)],
            dst_ref=RX.at[group, pl.ds(pl.multiple_of(p * CH, CH), CH)],
            send_sem=a1s.at[group, j], recv_sem=a1r.at[group, p],
            device_id={"tm": chip * 2 + pc, "series": pg}, device_id_type=MESH,
        ).wait_recv()

    def local_rows(group, core):
        return rows_of(group, core) - core * R

    def back_copy(group, j):
        pg = lax.rem(g + j, groups)
        row = pl.multiple_of(local_rows(group, c) + g * CH, CH)
        return pltpu.make_async_remote_copy(
            src_ref=CB.at[group, pl.ds(2 * pg, 2)],
            dst_ref=mix_out.at[:, pl.ds(row, CH), :],
            send_sem=a2s.at[group, j], recv_sem=a2r.at[group, g],
            device_id={"series": pg}, device_id_type=MESH,
        )

    def back_arrived(group, j):
        pg = lax.rem(g + j, groups)
        row = pl.multiple_of(local_rows(group, c) + pg * CH, CH)
        pltpu.make_async_remote_copy(
            src_ref=CB.at[group, pl.ds(0, 2)],
            dst_ref=mix_out.at[:, pl.ds(row, CH), :],
            send_sem=a2s.at[group, j], recv_sem=a2r.at[group, pg],
            device_id={"series": pg}, device_id_type=MESH,
        ).wait_recv()

    def hidden_copy(group):
        src = pl.multiple_of(rows_of(group, other), RC)
        dst = pl.multiple_of(local_rows(group, other), RC)
        return pltpu.make_async_remote_copy(
            src_ref=HID.at[pl.ds(src, RC)], dst_ref=hid_out.at[c, pl.ds(dst, RC)],
            send_sem=hs_sem.at[group, 0], recv_sem=hs_sem.at[group, 1],
            device_id={"tm": sib}, device_id_type=MESH,
        )

    def hidden_keep(group):
        src = pl.multiple_of(rows_of(group, c), RC)
        dst = pl.multiple_of(local_rows(group, c), RC)
        return pltpu.make_async_copy(
            HID.at[pl.ds(src, RC)], hid_out.at[c, pl.ds(dst, RC)], loc_sem.at[4 + group]
        )

    def mixed_keep(group):
        row = pl.multiple_of(local_rows(group, c) + g * CH, CH)
        return pltpu.make_async_copy(
            CB.at[group, pl.ds(2 * g, 2)], mix_out.at[:, pl.ds(row, CH), :], loc_sem.at[6 + group]
        )

    def finish_rows(group, rows, cores):
        wide = min(2 * tile, C)

        @pl.loop(0, D // wide)
        def _(j):
            cols = pl.ds(pl.multiple_of(j * wide, wide), wide)
            own_x = stacked(X, rows, cols)
            update = nn_dot(stacked(ATT, rows), wo[:, cols])
            scatter(HID, rows, cols, (own_x.astype(F32) + update).astype(BF16))

        if cores[-1] == 1:
            hidden_copy(group).start()
            hidden_keep(group).start()

        @pl.loop(0, C // wide)
        def _(j):
            cols = pl.ds(pl.multiple_of(j * wide, wide), wide)
            scatter(BR, rows, cols, nn_dot(stacked(HID, rows), wd[:, cols]).astype(BF16))

        for core in cores:
            plus = lax.rem(c + core, 2)

            @pl.when(plus == 0)
            def _():
                row = pl.multiple_of(rows_of(group, c) + g * CH, CH)
                RX[group, pl.ds(pl.multiple_of(mine * CH, CH), CH), :] = BR[pl.ds(row, CH), :]

            @pl.when(plus == 1)
            def _():
                spread_copy(group, 1).start()

            for i in range(1, groups):
                spread_copy(group, 2 * i + plus).start()

    def mix_rows(group):
        for j in range(1, members):
            spread_arrived(group, j)
        CB[group] = nn_dot(KR[...], RX[group]).astype(BF16).reshape(members, CH, C)
        for j in range(1, groups):
            back_copy(group, j).start()
        mixed_keep(group).start()

    mid_rows = [(RC, R)]
    out_rows = [(0, RC), (R + RC, RC)]
    for k in range(2):
        halo_arrived(0, k)
    project([(B, B)], False)
    attend(near_out, False, False)
    halo_arrived(1, 0)
    project([(2 * B + RC, R)], False)
    attend(mid, False, True)
    loads[1].wait()
    loads[2].wait()
    finish_rows(0, mid_rows, (0, 1))
    halo_arrived(1, 1)
    project([(halo_row(1, 0, 1), RC), (halo_row(1, 1, 1), RC)], False)
    for core in range(2):
        attend(far_out[core:core + 1], False, True)
        finish_rows(1, out_rows[core:core + 1], (core,))
    mix_rows(0)
    mix_rows(1)
    for group in range(2):
        hidden_copy(group).wait_recv()
        hidden_keep(group).wait()
        mixed_keep(group).wait()
        for j in range(1, groups):
            back_arrived(group, j)

    sib_copy.wait_send()
    halo_sent(0, 1)
    for k in range(2):
        halo_sent(1, k)
    for group in range(2):
        hidden_copy(group).wait_send()
        for j in range(1, members):
            spread_copy(group, j).wait_send()
        for j in range(1, groups):
            back_copy(group, j).wait_send()


def on_device(
    history, lengths, head_window, input_proj, output_proj, mixer_down, mixer_up, series_mix
):
    S, R, D = history.shape
    C = mixer_down.shape[1]
    chips = lax.axis_size("tm") // 2
    groups = lax.axis_size("series")
    members = 2 * groups
    B = 2 * R
    RC = R // 2
    CH = RC // groups
    pairs = D // PAIR
    smem = pl.BlockSpec(memory_space=pltpu.SMEM)
    vmem = pl.BlockSpec(memory_space=pltpu.VMEM)
    hbm = pl.BlockSpec(memory_space=pl.ANY)
    dma = pltpu.SemaphoreType.DMA
    hidden, mixed = pl.pallas_call(
        functools.partial(layer_kernel, (chips, groups)),
        out_shape=(
            jax.ShapeDtypeStruct((S, R, D), BF16), jax.ShapeDtypeStruct((S, R, C), BF16)
        ),
        in_specs=[smem, smem, vmem, hbm, hbm, hbm, hbm],
        out_specs=(hbm, hbm),
        scratch_shapes=[
            pltpu.VMEM((3 * B, D), BF16),
            pltpu.VMEM((B, D), BF16),
            pltpu.VMEM((3 * B, D), BF16),
            pltpu.VMEM((3 * B, 2 * D), BF16),
            pltpu.VMEM((pairs, 2, B, PAIR), F32),
            pltpu.VMEM((B, D), F32),
            pltpu.VMEM((B, D), F32),
            pltpu.VMEM((B, B), jnp.int32),
            pltpu.VMEM((R, B - RC), jnp.int32),
            pltpu.VMEM((R, B + RC), jnp.int32),
            pltpu.VMEM((R, R), jnp.int32),
            pltpu.VMEM((B, B + RC), F32),
            pltpu.VMEM((B, B + RC), F32),
            pltpu.VMEM((B, PAIR), F32),
            pltpu.VMEM((B, PAIR), F32),
            pltpu.VMEM((B, D), BF16),
            pltpu.VMEM((B, D), BF16),
            pltpu.VMEM((B, C), BF16),
            pltpu.VMEM((2, members * CH, C), BF16),
            pltpu.VMEM((members * CH, members * CH), BF16),
            pltpu.VMEM((2, members, CH, C), BF16),
            pltpu.VMEM(input_proj.shape, BF16),
            pltpu.VMEM(output_proj.shape, BF16),
            pltpu.VMEM(mixer_down.shape, BF16),
            dma((8,)), dma((2,)), dma((2, 2)), dma((2, 2, 2)), dma((2, 2, 2)),
            dma((2, members)), dma((2, members)), dma((2, groups)), dma((2, groups)),
        ],
        compiler_params=pltpu.CompilerParams(
            collective_id=0, has_side_effects=True, vmem_limit_bytes=64 * 1024 * 1024 - 65536
        ),
        name="layer",
    )(lengths, head_window, series_mix, history, input_proj, output_proj, mixer_down)
    update = jnp.einsum("spc,cd->spd", mixed, mixer_up, preferred_element_type=F32)
    return (hidden.astype(F32) + update).astype(BF16)


def solution(mesh):
    in_specs = (P("series", "tm", None), P("series"), P(), P(), P(), P(), P(), P())
    out_specs = P("series", "tm", None)
    return jax.shard_map(
        on_device, mesh=mesh, in_specs=in_specs, out_specs=out_specs, check_vma=False
    )
```

```python
import functools
import math

import jax
import jax.numpy as jnp
from jax import lax
from jax.experimental import pallas as pl
from jax.experimental.pallas import tpu as pltpu
from jax.sharding import PartitionSpec as P

HEAD_SIZE = 64
PAIR = 2 * HEAD_SIZE
NEG = -1e30
FAR = 1 << 20
MESH = pl.DeviceIdType.MESH
BF16 = jnp.bfloat16
F32 = jnp.float32
SCALE = HEAD_SIZE ** -0.5 * math.log2(math.e)


def nt_dot(a, b):
    return lax.dot_general(a, b, (((1,), (1,)), ((), ())), preferred_element_type=F32)


def nn_dot(a, b):
    return jnp.dot(a, b, preferred_element_type=F32)


def layer_kernel(
    dims, lengths, window, mix, hist, wi_any, wo_any, wd_any, hid_out, mix_out,
    X, Q, K, VO, M, L, ACC, DIST, DNO, DMID, DOUT, S0, S1, T0, T1, ATT, HID, BR, RX, KR, CB,
    wi, wo, wd,
    loc_sem, sib_sem, hs_sem, rs_sem, rr_sem, a1s, a1r, a2s, a2r,
):
    chips, groups = dims
    members = 2 * groups
    _, R, D = hist.shape
    B = 2 * R
    RC = R // 2
    C = BR.shape[1]
    CH = RC // groups
    pairs = D // PAIR
    me = lax.axis_index("tm")
    g = lax.axis_index("series")
    c = lax.rem(me, 2)
    chip = me // 2
    other = 1 - c
    sib = chip * 2 + other
    mine = g * 2 + c
    rchip = lax.rem(chip + 1, chips)
    lchip = lax.rem(chip + chips - 1, chips)
    total = chips * B
    has_left = chip > 0
    has_right = chip < chips - 1

    def member(j):
        p = lax.rem(mine + j, members)
        return p, p // 2, lax.rem(p, 2)

    barrier = pltpu.get_barrier_semaphore()
    for nchip in (lchip, rchip):
        for core in range(2):
            pl.semaphore_signal(
                barrier, inc=1, device_id={"tm": nchip * 2 + core}, device_id_type=MESH
            )
    for j in range(1, members):
        _, pg, pc = member(j)
        pl.semaphore_signal(
            barrier, inc=1, device_id={"tm": chip * 2 + pc, "series": pg}, device_id_type=MESH
        )
    own_rows = pl.multiple_of(c * R, R)
    own_load = pltpu.make_async_copy(hist.at[c], X.at[pl.ds(own_rows, R)], loc_sem.at[0])
    own_load.start()
    loads = [
        pltpu.make_async_copy(src, dst, loc_sem.at[1 + i])
        for i, (src, dst) in enumerate(((wi_any, wi), (wo_any, wo), (wd_any, wd)))
    ]
    loads[0].start()
    pl.semaphore_wait(barrier, 4 + members - 1)

    sib_copy = pltpu.make_async_remote_copy(
        src_ref=hist.at[other], dst_ref=X.at[pl.ds(own_rows, R)],
        send_sem=sib_sem.at[0], recv_sem=sib_sem.at[1],
        device_id={"tm": sib}, device_id_type=MESH,
    )
    sib_copy.start()

    sends = (
        jnp.where(c == 1, has_right, has_left),
        jnp.where(c == 1, has_left, has_right),
    )

    def halo_copy(phase, k, s):
        if phase == 0:
            target = jnp.where(c == 1, rchip, lchip)
            side = 1 - c
            kk = k + c * (1 - 2 * k)
            base = B + side * R
        else:
            target = jnp.where(c == 1, lchip, rchip)
            side = c
            kk = (1 - k) + c * (2 * k - 1)
            base = 2 * B + side * R
        row = pl.multiple_of(base + kk * RC, RC)
        return pltpu.make_async_remote_copy(
            src_ref=hist.at[s, pl.ds(pl.multiple_of(kk * RC, RC), RC)],
            dst_ref=X.at[pl.ds(row, RC)],
            send_sem=rs_sem.at[phase, k, s], recv_sem=rr_sem.at[phase, side, k],
            device_id={"tm": target * 2 + s}, device_id_type=MESH,
        )

    def halo_row(phase, side, k):
        return (phase + 1) * B + side * R + ((1 - k) if side == 0 else k) * RC

    def halo_arrived(phase, k):
        for side in range(2):
            @pl.when((has_left, has_right)[side])
            def _():
                pltpu.make_async_remote_copy(
                    src_ref=hist.at[0, pl.ds(0, RC)],
                    dst_ref=X.at[pl.ds(halo_row(phase, side, k), RC)],
                    send_sem=rs_sem.at[phase, k, 0], recv_sem=rr_sem.at[phase, side, k],
                    device_id={"tm": sib}, device_id_type=MESH,
                ).wait_recv()

    def start_halo(phase):
        @pl.when(sends[phase])
        def _():
            for k in range(2):
                for s in range(2):
                    halo_copy(phase, k, s).start()

    def halo_sent(phase, k):
        @pl.when(sends[phase])
        def _():
            for s in range(2):
                halo_copy(phase, k, s).wait_send()

    start_halo(0)
    for load in loads[1:]:
        load.start()

    @pl.when(jnp.logical_not(has_left))
    def _():
        for phase in range(1, 3):
            X[phase * B:phase * B + R, :] = jnp.zeros((R, D), BF16)

    @pl.when(jnp.logical_not(has_right))
    def _():
        for phase in range(1, 3):
            X[phase * B + R:(phase + 1) * B, :] = jnp.zeros((R, D), BF16)

    for p in range(pairs):
        VO[:, p * 2 * PAIR + PAIR:(p + 1) * 2 * PAIR] = jnp.ones((3 * B, PAIR), BF16)

    tile = 256

    def stacked(ref, rows, cols=slice(None)):
        parts = [ref[pl.ds(first, count), cols] for first, count in rows]
        return parts[0] if len(parts) == 1 else jnp.concatenate(parts, axis=0)

    def scatter(ref, rows, cols, value):
        at = 0
        for first, count in rows:
            ref[pl.ds(first, count), cols] = value[at:at + count]
            at += count

    def project(rows, with_queries):
        @pl.loop(0, D // tile)
        def _(j):
            cols = pl.ds(pl.multiple_of(j * tile, tile), tile)
            x = stacked(X, rows)
            if with_queries:
                scatter(Q, rows, cols, (nn_dot(x, wi[:, cols]) * SCALE).astype(BF16))
            kcols = pl.ds(pl.multiple_of(D + j * tile, tile), tile)
            scatter(K, rows, cols, nn_dot(x, wi[:, kcols]).astype(BF16))
            wcols = pl.ds(pl.multiple_of(2 * D + j * tile, tile), tile)
            values = nn_dot(x, wi[:, wcols]).astype(BF16)
            for i in range(tile // PAIR):
                at = pl.multiple_of((j * (tile // PAIR) + i) * 2 * PAIR, 2 * PAIR)
                scatter(VO, rows, pl.ds(at, PAIR), values[:, i * PAIR:(i + 1) * PAIR])

    length = lengths[c]
    first_valid = total - length

    def distances(unit):
        q_first, n, _, segments, ref, at = unit
        column = 0
        for k_first, k_count in segments:
            qi = q_first + lax.broadcasted_iota(jnp.int32, (n, k_count), 0)
            kj = k_first + lax.broadcasted_iota(jnp.int32, (n, k_count), 1)
            kpos = chip * B + kj
            valid = (kpos >= first_valid) & (kpos < total) & (kpos >= 0)
            ref[at:at + n, column:column + k_count] = jnp.where(valid, jnp.abs(qi - kj), FAR)
            column += k_count

    def pair_cols(hp):
        return pl.ds(pl.multiple_of(hp * PAIR, PAIR), PAIR)

    def scores(unit, hp, S, T, r0=0):
        q_first, n, ranges, _, ref, at = unit
        count = sum(k_count for _, k_count in ranges)
        low = lax.broadcasted_iota(jnp.int32, (n, PAIR), 1) < HEAD_SIZE
        cols = pair_cols(hp)
        q = Q[q_first:q_first + n, cols]
        zero = jnp.zeros_like(q)
        both = jnp.concatenate([jnp.where(low, q, zero), jnp.where(low, zero, q)], axis=0)
        parts = [nt_dot(both, K[k_row:k_row + k_count, cols]) for k_row, k_count in ranges]
        s = parts[0] if len(parts) == 1 else jnp.concatenate(parts, axis=1)
        dist = ref[at:at + n, :count]
        s = jnp.concatenate([
            jnp.where(dist <= window[2 * hp], s[:n], NEG),
            jnp.where(dist <= window[2 * hp + 1], s[n:], NEG),
        ], axis=0)
        S[r0:r0 + 2 * n, :count] = s
        lanes = min(PAIR, count)
        T[r0:r0 + 2 * n, :lanes] = functools.reduce(
            jnp.maximum, [s[:, i:i + lanes] for i in range(0, count, lanes)]
        )

    def values(unit, hp, S, T, first, last, r0=0):
        q_first, n, ranges, _, _, _ = unit
        count = sum(k_count for _, k_count in ranges)
        low = lax.broadcasted_iota(jnp.int32, (n, PAIR), 1) < HEAD_SIZE
        cols = pair_cols(hp)
        vcols = pl.ds(pl.multiple_of(hp * 2 * PAIR, 2 * PAIR), 2 * PAIR)
        q_rows = slice(q_first, q_first + n)
        lanes = min(PAIR, count)
        top = jnp.max(T[r0:r0 + 2 * n, :lanes], axis=1, keepdims=True)
        top = jnp.broadcast_to(top, (2 * n, PAIR))
        if not first:
            old = jnp.concatenate([M[hp, 0, q_rows, :], M[hp, 1, q_rows, :]], axis=0)
            top = jnp.maximum(top, old)
        added = None
        column = 0
        for k_row, k_count in ranges:
            step = min(PAIR, k_count)
            p = jnp.concatenate([
                jnp.exp2(S[r0:r0 + 2 * n, i:i + step] - top[:, :step]).astype(BF16)
                for i in range(column, column + k_count, step)
            ], axis=1)
            part = nn_dot(p, VO[k_row:k_row + k_count, vcols])
            added = part if added is None else added + part
            column += k_count
        acc = jnp.where(low, added[:n, :PAIR], added[n:, :PAIR])
        sums = jnp.where(low, added[:n, PAIR:], added[n:, PAIR:])
        if not first:
            alpha = jnp.exp2(jnp.where(low, old[:n] - top[:n], old[n:] - top[n:]))
            acc = acc + ACC[q_rows, cols] * alpha
            sums = sums + L[q_rows, cols] * alpha
        if last:
            qpos = chip * B + q_first + lax.broadcasted_iota(jnp.int32, (n, PAIR), 0)
            ATT[q_rows, cols] = jnp.where(qpos >= first_valid, acc / sums, 0.0).astype(BF16)
        else:
            M[hp, 0, q_rows, :] = top[:n]
            M[hp, 1, q_rows, :] = top[n:]
            ACC[q_rows, cols] = acc
            L[q_rows, cols] = sums

    def attend(units, first, last, start=0, stop=None):
        if len(units) == 1:
            batches = [[(units[0], 2 * i + b, 2 * RC * b) for b in range(2)] for i in range(2)]
            step = 4
        elif units[0][1] == R:
            batches = [[(units[0], 0, 0)], [(units[1], 0, 0)]]
            step = 1
        else:
            batches = [[(unit, i, 2 * RC * b) for b, unit in enumerate(units)] for i in range(2)]
            step = 2

        def all_scores(batch, hp, S, T):
            for unit, plus, r0 in batch:
                scores(unit, hp + plus, S, T, r0)

        def all_values(batch, hp, S, T):
            for unit, plus, r0 in batch:
                values(unit, hp + plus, S, T, first, last, r0)

        if start == 0:
            all_scores(batches[0], 0, S0, T0)
        stop = pairs if stop is None else stop

        @pl.loop(start // step, stop // step)
        def _(i):
            hp = i * step
            all_scores(batches[1], hp, S1, T1)
            all_values(batches[0], hp, S0, T0)
            all_scores(batches[0], jnp.minimum(hp + step, pairs - step), S0, T0)
            all_values(batches[1], hp, S1, T1)

    own = [(b * R, R, ((0, B),), ((0, B),), DIST, b * R) for b in range(2)]
    near_out = [
        (0, RC, ((B, B - RC),), ((-R, R), (B, RC)), DNO, 0),
        (R + RC, RC, ((B + RC, B - RC),), ((-RC, RC), (B, R)), DNO, RC),
    ]
    near_segments = ((-R, R), (B, R))
    mid = [
        (RC, RC, ((B, B), (2 * B + RC, RC)), near_segments + ((-B + RC, RC),), DMID, 0),
        (R, RC, ((B, B), (2 * B + R, RC)), near_segments + ((B + R, RC),), DMID, RC),
    ]
    far_out = [
        (0, RC, ((2 * B, R),), ((-B, R),), DOUT, 0),
        (R + RC, RC, ((2 * B + R, R),), ((B + R, R),), DOUT, RC),
    ]

    own_load.wait()
    loads[0].wait()
    project([(own_rows, R)], True)
    for unit in own + near_out + mid + far_out:
        distances(unit)

    n = members * CH
    row_i = lax.broadcasted_iota(jnp.int32, (n, members), 0)
    col_t = lax.broadcasted_iota(jnp.int32, (n, members), 1)
    spread = jnp.where(
        (row_i >= col_t * CH) & (row_i < (col_t + 1) * CH), 1.0, 0.0
    ).astype(BF16)
    half_mix = nn_dot(spread, mix[...]).astype(BF16)
    full_mix = nt_dot(half_mix, spread)
    i2 = lax.broadcasted_iota(jnp.int32, (n, n), 0) & (CH - 1)
    j2 = lax.broadcasted_iota(jnp.int32, (n, n), 1) & (CH - 1)
    KR[...] = jnp.where(i2 == j2, full_mix, 0.0).astype(BF16)

    sib_copy.wait_recv()
    project([(pl.multiple_of(other * R, R), R)], True)
    part = pairs // 4
    attend(own, True, False, 0, part)
    halo_sent(0, 0)
    start_halo(1)
    attend(own, True, False, part)

    def rows_of(group, core):
        return (RC + core * RC) if group == 0 else core * (R + RC)

    def spread_copy(group, j):
        p, pg, pc = member(j)
        row = pl.multiple_of(rows_of(group, pc) + pg * CH, CH)
        return pltpu.make_async_remote_copy(
            src_ref=BR.at[pl.ds(row, CH)],
            dst_ref=RX.at[group, pl.ds(pl.multiple_of(mine * CH, CH), CH)],
            send_sem=a1s.at[group, j], recv_sem=a1r.at[group, mine],
            device_id={"tm": chip * 2 + pc, "series": pg}, device_id_type=MESH,
        )

    def spread_arrived(group, j):
        p, pg, pc = member(j)
        pltpu.make_async_remote_copy(
            src_ref=BR.at[pl.ds(0, CH)],
            dst_ref=RX.at[group, pl.ds(pl.multiple_of(p * CH, CH), CH)],
            send_sem=a1s.at[group, j], recv_sem=a1r.at[group, p],
            device_id={"tm": chip * 2 + pc, "series": pg}, device_id_type=MESH,
        ).wait_recv()

    def local_rows(group, core):
        return rows_of(group, core) - core * R

    def back_copy(group, j):
        pg = lax.rem(g + j, groups)
        row = pl.multiple_of(local_rows(group, c) + g * CH, CH)
        return pltpu.make_async_remote_copy(
            src_ref=CB.at[group, pl.ds(2 * pg, 2)],
            dst_ref=mix_out.at[:, pl.ds(row, CH), :],
            send_sem=a2s.at[group, j], recv_sem=a2r.at[group, g],
            device_id={"series": pg}, device_id_type=MESH,
        )

    def back_arrived(group, j):
        pg = lax.rem(g + j, groups)
        row = pl.multiple_of(local_rows(group, c) + pg * CH, CH)
        pltpu.make_async_remote_copy(
            src_ref=CB.at[group, pl.ds(0, 2)],
            dst_ref=mix_out.at[:, pl.ds(row, CH), :],
            send_sem=a2s.at[group, j], recv_sem=a2r.at[group, pg],
            device_id={"series": pg}, device_id_type=MESH,
        ).wait_recv()

    def hidden_copy(group):
        src = pl.multiple_of(rows_of(group, other), RC)
        dst = pl.multiple_of(local_rows(group, other), RC)
        return pltpu.make_async_remote_copy(
            src_ref=HID.at[pl.ds(src, RC)], dst_ref=hid_out.at[c, pl.ds(dst, RC)],
            send_sem=hs_sem.at[group, 0], recv_sem=hs_sem.at[group, 1],
            device_id={"tm": sib}, device_id_type=MESH,
        )

    def hidden_keep(group):
        src = pl.multiple_of(rows_of(group, c), RC)
        dst = pl.multiple_of(local_rows(group, c), RC)
        return pltpu.make_async_copy(
            HID.at[pl.ds(src, RC)], hid_out.at[c, pl.ds(dst, RC)], loc_sem.at[4 + group]
        )

    def mixed_keep(group):
        row = pl.multiple_of(local_rows(group, c) + g * CH, CH)
        return pltpu.make_async_copy(
            CB.at[group, pl.ds(2 * g, 2)], mix_out.at[:, pl.ds(row, CH), :], loc_sem.at[6 + group]
        )

    def finish_rows(group, rows, cores):
        wide = min(2 * tile, C)

        @pl.loop(0, D // wide)
        def _(j):
            cols = pl.ds(pl.multiple_of(j * wide, wide), wide)
            own_x = stacked(X, rows, cols)
            update = nn_dot(stacked(ATT, rows), wo[:, cols])
            scatter(HID, rows, cols, (own_x.astype(F32) + update).astype(BF16))

        if cores[-1] == 1:
            hidden_copy(group).start()
            hidden_keep(group).start()

        @pl.loop(0, C // wide)
        def _(j):
            cols = pl.ds(pl.multiple_of(j * wide, wide), wide)
            scatter(BR, rows, cols, nn_dot(stacked(HID, rows), wd[:, cols]).astype(BF16))

        for core in cores:
            plus = lax.rem(c + core, 2)

            @pl.when(plus == 0)
            def _():
                row = pl.multiple_of(rows_of(group, c) + g * CH, CH)
                RX[group, pl.ds(pl.multiple_of(mine * CH, CH), CH), :] = BR[pl.ds(row, CH), :]

            @pl.when(plus == 1)
            def _():
                spread_copy(group, 1).start()

            for i in range(1, groups):
                spread_copy(group, 2 * i + plus).start()

    def mix_rows(group):
        for j in range(1, members):
            spread_arrived(group, j)
        CB[group] = nn_dot(KR[...], RX[group]).astype(BF16).reshape(members, CH, C)
        for j in range(1, groups):
            back_copy(group, j).start()
        mixed_keep(group).start()

    mid_rows = [(RC, R)]
    out_rows = [(0, RC), (R + RC, RC)]
    for k in range(2):
        halo_arrived(0, k)
    project([(B, B)], False)
    attend(near_out, False, False)
    halo_arrived(1, 0)
    project([(2 * B + RC, R)], False)
    attend(mid, False, True)
    loads[1].wait()
    loads[2].wait()
    finish_rows(0, mid_rows, (0, 1))
    halo_arrived(1, 1)
    project([(halo_row(1, 0, 1), RC), (halo_row(1, 1, 1), RC)], False)
    for core in range(2):
        attend(far_out[core:core + 1], False, True)
        finish_rows(1, out_rows[core:core + 1], (core,))
    mix_rows(0)
    mix_rows(1)
    for group in range(2):
        hidden_copy(group).wait_recv()
        hidden_keep(group).wait()
        mixed_keep(group).wait()
        for j in range(1, groups):
            back_arrived(group, j)

    sib_copy.wait_send()
    halo_sent(0, 1)
    for k in range(2):
        halo_sent(1, k)
    for group in range(2):
        hidden_copy(group).wait_send()
        for j in range(1, members):
            spread_copy(group, j).wait_send()
        for j in range(1, groups):
            back_copy(group, j).wait_send()


def on_device(
    history, lengths, head_window, input_proj, output_proj, mixer_down, mixer_up, series_mix
):
    S, R, D = history.shape
    C = mixer_down.shape[1]
    chips = lax.axis_size("tm") // 2
    groups = lax.axis_size("series")
    members = 2 * groups
    B = 2 * R
    RC = R // 2
    CH = RC // groups
    pairs = D // PAIR
    smem = pl.BlockSpec(memory_space=pltpu.SMEM)
    vmem = pl.BlockSpec(memory_space=pltpu.VMEM)
    hbm = pl.BlockSpec(memory_space=pl.ANY)
    dma = pltpu.SemaphoreType.DMA
    hidden, mixed = pl.pallas_call(
        functools.partial(layer_kernel, (chips, groups)),
        out_shape=(
            jax.ShapeDtypeStruct((S, R, D), BF16), jax.ShapeDtypeStruct((S, R, C), BF16)
        ),
        in_specs=[smem, smem, vmem, hbm, hbm, hbm, hbm],
        out_specs=(hbm, hbm),
        scratch_shapes=[
            pltpu.VMEM((3 * B, D), BF16),
            pltpu.VMEM((B, D), BF16),
            pltpu.VMEM((3 * B, D), BF16),
            pltpu.VMEM((3 * B, 2 * D), BF16),
            pltpu.VMEM((pairs, 2, B, PAIR), F32),
            pltpu.VMEM((B, D), F32),
            pltpu.VMEM((B, D), F32),
            pltpu.VMEM((B, B), jnp.int32),
            pltpu.VMEM((R, B - RC), jnp.int32),
            pltpu.VMEM((R, B + RC), jnp.int32),
            pltpu.VMEM((R, R), jnp.int32),
            pltpu.VMEM((B, B + RC), F32),
            pltpu.VMEM((B, B + RC), F32),
            pltpu.VMEM((B, PAIR), F32),
            pltpu.VMEM((B, PAIR), F32),
            pltpu.VMEM((B, D), BF16),
            pltpu.VMEM((B, D), BF16),
            pltpu.VMEM((B, C), BF16),
            pltpu.VMEM((2, members * CH, C), BF16),
            pltpu.VMEM((members * CH, members * CH), BF16),
            pltpu.VMEM((2, members, CH, C), BF16),
            pltpu.VMEM(input_proj.shape, BF16),
            pltpu.VMEM(output_proj.shape, BF16),
            pltpu.VMEM(mixer_down.shape, BF16),
            dma((8,)), dma((2,)), dma((2, 2)), dma((2, 2, 2)), dma((2, 2, 2)),
            dma((2, members)), dma((2, members)), dma((2, groups)), dma((2, groups)),
        ],
        compiler_params=pltpu.CompilerParams(
            collective_id=0, has_side_effects=True, vmem_limit_bytes=64 * 1024 * 1024 - 65536
        ),
        name="layer",
    )(lengths, head_window, series_mix, history, input_proj, output_proj, mixer_down)
    update = jnp.einsum("spc,cd->spd", mixed, mixer_up, preferred_element_type=F32)
    return (hidden.astype(F32) + update).astype(BF16)


def solution(mesh):
    in_specs = (P("series", "tm", None), P("series"), P(), P(), P(), P(), P(), P())
    out_specs = P("series", "tm", None)
    return jax.shard_map(
        on_device, mesh=mesh, in_specs=in_specs, out_specs=out_specs, check_vma=False
    )
```
